256 devices in a mesh: grp: 16 (over x, y_hi, core), mem: 16 (over z, y_lo).
Axes of the slice: x: 4, y: 4 (y_hi: 2, y_lo: 2; y = y_hi * 2 + y_lo), z: 8, core: 2. Of those that a mesh axis runs over, the one named last changes fastest.
Arguments:
- residual: float32 [2048, 64, 256], P(('grp', 'mem')), may hold values from -6 to 6
- direction: float32 [2048, 64, 256], P(('grp', 'mem')), may hold values from -6 to 6
- local_inverse: bfloat16 [2048, 256, 256], P(('grp', 'mem')), may hold values from -1 to 16, as said below
- dirichlet: bfloat16 [2048, 256, 256], P(('grp', 'mem')), may hold values from -1 to 16, as said below
- coupling: bfloat16 [2048, 24, 256], P(('grp', 'mem')), may hold values from -0.375 to 0.375
- corner_map: int32 [2048, 24], P(('grp', 'mem')), may hold values from 0 to 6143
- coarse_factor: bfloat16 [16, 2048, 2048], P('grp'), may hold values from -1 to 3, as said below
Outputs:
- new_residual: float32 [2048, 64, 256], P(('grp', 'mem'))
- new_direction: float32 [2048, 64, 256], P(('grp', 'mem'))
- step_sizes: float32 [3, 64], replicated
The draws below stay inside these ranges and needn't reach their ends.
Inputs may be any that keep to these rules, and one draw needn't show every extreme that they name: `local_inverse`: each subdomain's matrix is symmetric positive definite. `dirichlet`: each subdomain's matrix is symmetric positive definite. `coarse_factor`: each group's factor is lower triangular with a positive diagonal.
All inputs are finite; a program needn't handle non-finite values.
Results may differ from the reference program's by a relative error of at most 0.0083.
Values sent between devices are 32-bit elements; how exact they have to be, the bound alone decides.
A program may use at most 128 MiB of HBM per device.

```python
import jax
import jax.numpy as jnp
from jax import lax

SUB = 8
NR = 256
NC = 24
Q = 64
NCO = 2048
ITERS = 3
SUBS = 2048
N_GRP = 16
N_MEM = 16


def spd_blocks(key, count, order):
    first_key, second_key = jax.random.split(key, 2)
    diagonal = jnp.exp(jax.random.uniform(first_key, (count, order), jnp.float32, jnp.log(1.5), jnp.log(4.0)))
    spread = 0.5 * (3.0 / order) ** 0.5
    raw_values = jax.random.uniform(second_key, (count, order, order), jnp.float32, -spread, spread)
    upper_part = jnp.triu(raw_values, 1)
    matrices = upper_part + jnp.swapaxes(upper_part, 1, 2) + diagonal[:, :, None] * jnp.eye(order, dtype=jnp.float32)
    return matrices


def draw_local_inverse(key, part):
    return spd_blocks(jax.random.fold_in(key, 11), SUBS, NR).astype(jnp.bfloat16)


def draw_dirichlet(key, part):
    return spd_blocks(jax.random.fold_in(key, 12), SUBS, NR).astype(jnp.bfloat16)


def draw_coarse_factor(key, part):
    first_key, second_key = jax.random.split(jax.random.fold_in(key, 13))
    upper_diag = 2.0
    spread = 0.6 * (3.0 / NCO) ** 0.5
    diagonal = jnp.exp(jax.random.uniform(first_key, (N_GRP, NCO), jnp.float32, 0.0, jnp.log(upper_diag)))
    raw_values = jax.random.uniform(second_key, (N_GRP, NCO, NCO), jnp.float32, -spread, spread)
    factor = jnp.tril(raw_values, -1) + diagonal[:, :, None] * jnp.eye(NCO, dtype=jnp.float32)
    return factor.astype(jnp.bfloat16)


def plant(result, stream_key, smallest, largest):
    place = [jax.random.randint(jax.random.fold_in(stream_key, axis), (), 0, length) for axis, length in enumerate(result.shape)]
    longest = result.shape.index(max(result.shape))
    next_to = place[:longest] + [(place[longest] + 1) % result.shape[longest]] + place[longest + 1:]
    return result.at[tuple(place)].set(smallest).at[tuple(next_to)].set(largest)


def block_scale(own_key, dims, shards, smallest, largest):
    loudness, own = 1.0, jax.random.fold_in(own_key, 6)
    for dim, parts in shards:
        steps = jnp.exp(jax.random.uniform(jax.random.fold_in(own, dim), (parts,), jnp.float32, smallest / len(shards), largest / len(shards)))
        loudness = loudness * jnp.repeat(steps, dims[dim] // parts).reshape([-1 if axis == dim else 1 for axis in range(len(dims))])
    return loudness


def normal_values(rng, dims, deviation, limit, cuts=(), held_as=jnp.bfloat16):
    drawn = jax.random.normal(rng, dims, jnp.float32) * deviation
    if len(cuts) > 0:
        drawn = block_scale(rng, dims, cuts, -0.22, 0.18) * drawn
    return jnp.clip(drawn, min=-limit, max=limit).astype(held_as)


def setup_inputs(seed: int = 0) -> dict:
    streams_of = jax.random.split(jax.random.key(seed), 8)
    return {
        "residual": normal_values(streams_of[0], (SUBS, Q, NR), 1.0, 6.0, ((0, 256),), jnp.float32),
        "direction": normal_values(streams_of[1], (SUBS, Q, NR), 1.0, 6.0, ((0, 256),), jnp.float32),
        "local_inverse": draw_local_inverse(jax.random.fold_in(streams_of[7], 71), 0),
        "dirichlet": draw_dirichlet(jax.random.fold_in(streams_of[7], 71), 0),
        "coupling": normal_values(streams_of[4], (SUBS, NC, NR), NR ** -0.5, 0.375, ((0, 256),)),
        "corner_map": plant(jax.random.randint(streams_of[5], (SUBS, NC), 0, 3 * NCO), jax.random.fold_in(streams_of[5], 1), 0, (3 * NCO) - 1).astype(jnp.int32),
        "coarse_factor": draw_coarse_factor(jax.random.fold_in(streams_of[7], 71), 0),
    }


highest = lax.Precision.HIGHEST

def blockwise(matrices, vectors):
    devices = matrices.shape[0] // SUB
    matrix_blocks = matrices.reshape(devices, SUB, NR, NR)
    vector_blocks = vectors.astype(jnp.bfloat16).reshape(devices, SUB, Q, NR)

    def apply_one(operands):
        return jnp.einsum('sij,skj->ski', operands[0].astype(jnp.float32), operands[1].astype(jnp.float32), precision=highest)
    return lax.map(apply_one, (matrix_blocks, vector_blocks)).reshape(vectors.shape)

def coarse_solve(factor, coarse_load):
    forward = jax.scipy.linalg.solve_triangular(factor, coarse_load.T, lower=True)
    return jax.scipy.linalg.solve_triangular(factor, forward, lower=True, trans=1).T

def reference(residual, direction, local_inverse, dirichlet, coupling, corner_map, coarse_factor):
    coupling_wide = coupling.astype(jnp.float32)
    groups = jnp.arange(SUBS, dtype=jnp.int32) // (SUB * N_MEM)
    owner_row = (groups[:, None] + corner_map // NCO - 1) % N_GRP * NCO + corner_map % NCO
    flat_owner = owner_row.reshape(-1).astype(jnp.int32)
    factors = coarse_factor.astype(jnp.float32)
    precond = blockwise(dirichlet, residual)
    norm_now = jnp.sum(residual * precond, axis=(0, 2))
    step_list = []
    for iteration in range(ITERS):
        solved = blockwise(local_inverse, direction)
        partial_value = jnp.einsum('ski,sci->skc', solved, coupling_wide, precision=highest)
        coarse_load = jnp.zeros((Q, N_GRP * NCO), jnp.float32).at[:, flat_owner].add(partial_value.transpose(1, 0, 2).reshape(Q, SUBS * NC))
        blocks = coarse_load.reshape(Q, N_GRP, NCO).transpose(1, 0, 2)
        coarse = lax.map(lambda operands: coarse_solve(operands[0], operands[1]), (factors, blocks))
        coarse = coarse.transpose(1, 0, 2).reshape(Q, N_GRP * NCO)
        picked = coarse[:, flat_owner].reshape(Q, SUBS, NC).transpose(1, 0, 2)
        lifted = jnp.einsum('skc,sci->ski', picked, coupling_wide, precision=highest)
        image = blockwise(local_inverse, direction + lifted)
        curvature = jnp.sum(direction * image, axis=(0, 2))
        alpha = norm_now / curvature
        step_list.append(alpha)
        residual = residual - alpha[None, :, None] * image
        precond = blockwise(dirichlet, residual)
        norm_next = jnp.sum(residual * precond, axis=(0, 2))
        direction = precond + (norm_next / norm_now)[None, :, None] * direction
        norm_now = norm_next
    return (residual, direction, jnp.stack(step_list))
```

```python
import functools

import jax
import jax.numpy as jnp
from jax import lax
from jax.experimental import pallas as pl
from jax.experimental.pallas import tpu as pltpu
from jax.sharding import PartitionSpec as P

ITERS = 3
MESH = pl.DeviceIdType.MESH
F32, BF16 = jnp.float32, jnp.bfloat16
BLK = 256


def nn(a, b):
    return lax.dot_general(a, b, (((1,), (0,)), ((), ())), preferred_element_type=F32)


def nt(a, b):
    return lax.dot_general(a, b, (((1,), (1,)), ((), ())), preferred_element_type=F32)


def pieces(x):
    high = x.astype(BF16)
    return high, (x - high.astype(F32)).astype(BF16)


def iota(shape, dim):
    return lax.broadcasted_iota(jnp.int32, shape, dim)


def kernel(
    n_grp, n_mem,
    r_in, d_in, kmat, dmat, cst, idx, factor,
    r_ref, d_ref, steps_ref,
    img, l_ref, xh, xl, oht, mask, a_ref,
    snd, rcv, snd2, rcv2, idx_all, load, nbr, ext, ar,
    fsem, sem_i, sem_f, sem_b, sem_n, sem_x, sem_a,
):
    subs, q_all, _ = r_in.shape
    nb = l_ref.shape[0] // BLK
    rows4 = 4 * nb
    n_rows = 3 * rows4
    me, grp = lax.axis_index("mem"), lax.axis_index("grp")
    top = iota((8, 128), 0) < 4
    top2 = iota((8, BLK), 0) < 4
    band = iota((q_all, 128), 1) // 32

    fetch = pltpu.make_async_copy(factor.at[0], l_ref, fsem)
    fetch.start()

    barrier = pltpu.get_barrier_semaphore()
    for step in range(1, n_mem):
        pl.semaphore_signal(
            barrier, inc=1, device_id={"mem": lax.rem(me + step, n_mem)}, device_id_type=MESH
        )
    for step in range(1, n_grp):
        pl.semaphore_signal(
            barrier, inc=1, device_id={"grp": lax.rem(grp + step, n_grp)}, device_id_type=MESH
        )
    pl.semaphore_wait(barrier, n_mem + n_grp - 2)

    def to_member(src, dst, sem, step):
        return pltpu.make_async_remote_copy(
            src_ref=src, dst_ref=dst, send_sem=sem.at[0, step], recv_sem=sem.at[1, step],
            device_id={"mem": lax.rem(me + step, n_mem)}, device_id_type=MESH,
        )

    def to_group(src, dst, sem, step):
        return pltpu.make_async_remote_copy(
            src_ref=src, dst_ref=dst, send_sem=sem.at[0, step], recv_sem=sem.at[1, step],
            device_id={"grp": lax.rem(grp + step, n_grp)}, device_id_type=MESH,
        )

    idx_all[pl.ds(me, 1)] = idx[...][None]
    for step in range(1, n_mem):
        to_member(idx, idx_all.at[me], sem_i, step).start()

    def reduce_start(which, row):
        mine = ar.at[which, 0]
        mine[pl.ds(me, 1)] = row[None]
        for step in range(1, n_mem):
            to_member(mine.at[me], mine.at[me], sem_a.at[which, 0], step).start()

    def reduce_middle(which):
        mine, other = ar.at[which, 0], ar.at[which, 1]
        for step in range(1, n_mem):
            to_member(mine.at[me], mine.at[lax.rem(me + n_mem - step, n_mem)], sem_a.at[which, 0], step).wait()
        row = jnp.sum(mine[...], axis=0)
        other[pl.ds(grp, 1)] = row[None]
        for step in range(1, n_grp):
            to_group(other.at[grp], other.at[grp], sem_a.at[which, 1], step).start()

    def reduce_end(which):
        other = ar.at[which, 1]
        for step in range(1, n_grp):
            to_group(other.at[grp], other.at[lax.rem(grp + n_grp - step, n_grp)], sem_a.at[which, 1], step).wait()
        return jnp.sum(other[...], axis=0)

    def all_reduce(which, row):
        reduce_start(which, row)
        reduce_middle(which)
        return reduce_end(which)

    def as_row(total):
        wide = jnp.concatenate([total, jnp.zeros((128 - q_all, BLK), F32)], axis=0)
        first, rest = wide.astype(BF16), wide
        ones = jnp.ones((8, BLK), BF16)
        rest = rest - first.astype(F32)
        second = rest.astype(BF16)
        third = (rest - second.astype(F32)).astype(BF16)
        out = nt(ones, first) + (nt(ones, second) + nt(ones, third))
        return out[0:1]

    def as_column(row):
        diagonal = iota((q_all, 128), 0) == iota((q_all, 128), 1)
        return jnp.sum(jnp.where(diagonal, jnp.broadcast_to(row, (q_all, 128)), 0.0), axis=1, keepdims=True)

    def halves_to_tiles(p0, p1):
        for v in range(q_all // 8):
            a, b = p0[8 * v : 8 * v + 8], p1[8 * v : 8 * v + 8]
            snd[2 * v] = jnp.where(top, a, pltpu.roll(b, 4, 0))
            snd[2 * v + 1] = jnp.where(top, pltpu.roll(a, 4, 0), b)

    def send_partials():
        halves = []
        for h in range(2):
            stack = []
            for s in range(4 * h, 4 * h + 4):
                stack += pieces(nn(d_ref[s].astype(BF16), kmat[s]))
            found = nt(jnp.concatenate(stack, axis=0), cst[h])
            total = jnp.zeros((q_all, 128), F32)
            for s in range(4):
                part = found[2 * s * q_all : (2 * s + 1) * q_all] + found[(2 * s + 1) * q_all : (2 * s + 2) * q_all]
                total = jnp.where(band == s, part, total)
            halves.append(total)
        halves_to_tiles(*halves)
        for step in range(1, n_mem):
            to_member(snd.at[lax.rem(me + step, n_mem)], rcv.at[me], sem_f, step).start()
        rcv[pl.ds(me, 1)] = snd[pl.ds(me, 1)]

    def invert_blocks():
        fetch.wait()
        row, col = iota((BLK, BLK), 0), iota((BLK, BLK), 1)

        def one(i, carry):
            at = pl.multiple_of(i * BLK, BLK)
            tri = l_ref[pl.ds(at, BLK), pl.ds(at, BLK)].astype(F32)
            inv = jnp.where(row == col, 1.0 / jnp.where(row == col, tri, 1.0), 0.0)
            size = 1
            while size < BLK:
                below = (row // (2 * size) == col // (2 * size)) & (row // size > col // size)
                off = jnp.where(below, tri, 0.0).astype(BF16)
                high, low = pieces(inv)
                left = nn(high, off) + nn(low, off)
                left_high, left_low = pieces(left)
                inv = inv - (nn(left_high, high) + (nn(left_high, low) + nn(left_low, high)))
                size *= 2
            high, low = pieces(inv)
            xh[pl.ds(i, 1)] = high[None]
            xl[pl.ds(i, 1)] = low[None]
            return carry

        lax.fori_loop(0, nb, one, 0)

    def build_masks():
        for step in range(1, n_mem):
            to_member(idx, idx_all.at[lax.rem(me + n_mem - step, n_mem)], sem_i, step).wait()

        def one(j, carry):
            tile = idx_all[pl.ds(j, 1)][0]
            for h in range(2):
                line = tile[4 * h : 4 * h + 1]
                at = pl.multiple_of(j * BLK + h * 128, 128)
                lo = jnp.broadcast_to(line & (BLK - 1), (BLK, 128))
                oht[:, pl.ds(at, 128)] = jnp.where(lo == iota((BLK, 128), 0), 1.0, 0.0).astype(BF16)
                hi = jnp.broadcast_to(line >> 8, (n_rows, 128))
                mask[:, pl.ds(at, 128)] = jnp.where(hi == iota((n_rows, 128), 0) // 4, 1.0, 0.0)
            return carry

        lax.fori_loop(0, n_mem, one, 0)

    def scatter():
        for step in range(n_mem):
            j = lax.rem(me + n_mem - step, n_mem)
            if step:
                to_member(snd.at[lax.rem(me + step, n_mem)], rcv.at[j], sem_f, step).wait()
            tile = rcv[pl.ds(j, 1)][0]
            high = tile.astype(BF16).astype(F32)
            for number, part in enumerate((high, tile - high)):
                turned = pltpu.roll(part, 4, 0)
                for h in range(2):
                    twice = jnp.where(top, part, turned) if h == 0 else jnp.where(top, turned, part)
                    at = pl.multiple_of(j * BLK + h * 128, 128)
                    full = jnp.concatenate([twice] * (n_rows // 8), axis=0) * mask[:, pl.ds(at, 128)]
                    a_ref[number * n_rows : (number + 1) * n_rows, pl.ds(at, 128)] = full.astype(BF16)
        both = nt(a_ref[...], oht[...])
        load[...] = both[:n_rows] + both[n_rows:]

    def fold_neighbours():
        up = to_group(load.at[2 * rows4 : 3 * rows4], nbr.at[0], sem_n, 1)
        down = to_group(load.at[0:rows4], nbr.at[1], sem_n, n_grp - 1)
        up.start()
        down.start()
        up.wait()
        down.wait()
        return load[rows4 : 2 * rows4] + nbr[0] + nbr[1]

    def twin(x):
        high, low = pieces(x)
        return jnp.where(top2, high.astype(F32), low.astype(F32)).astype(BF16)

    def folded(x):
        return x + pltpu.roll(x, 4, 0)

    def coarse_solve(b):
        acc = []
        for v in range(nb // 2):
            x = b[8 * v : 8 * v + 8]
            y = pltpu.roll(x, 4, 0)
            acc += [jnp.where(top2, x, y), jnp.where(top2, y, x)]
        for i in range(nb):
            p = twin(acc[i])
            acc[i] = folded(nt(p, xh[i]) + nt(p, xl[i]))
            p = twin(acc[i])
            for t in range(i + 1, nb):
                acc[t] = acc[t] - folded(nt(p, l_ref[t * BLK : (t + 1) * BLK, i * BLK : (i + 1) * BLK]))
        for i in reversed(range(nb)):
            p = twin(acc[i])
            acc[i] = folded(nn(p, xh[i]) + nn(p, xl[i]))
            p = twin(acc[i])
            for t in range(i):
                acc[t] = acc[t] - folded(nn(p, l_ref[i * BLK : (i + 1) * BLK, t * BLK : (t + 1) * BLK]))
        for v in range(nb // 2):
            ext[rows4 + 8 * v : rows4 + 8 * v + 8] = jnp.where(top2, acc[2 * v], acc[2 * v + 1])

    def spread_neighbours():
        own = ext.at[rows4 : 2 * rows4]
        up = to_group(own, ext.at[0:rows4], sem_x, 1)
        down = to_group(own, ext.at[2 * rows4 : 3 * rows4], sem_x, n_grp - 1)
        up.start()
        down.start()
        up.wait()
        down.wait()

    def pick():
        high, low = pieces(ext[...])
        both = jnp.concatenate([high, low], axis=0)
        for step in list(range(1, n_mem)) + [0]:
            j = lax.rem(me + step, n_mem)
            at = pl.multiple_of(j * BLK, BLK)
            found = nn(both, oht[:, pl.ds(at, BLK)])
            found = (found[:n_rows] + found[n_rows:]) * mask[:, pl.ds(at, BLK)]
            total = found[0:8]
            for v in range(1, n_rows // 8):
                total = total + found[8 * v : 8 * v + 8]
            total = folded(total)
            tile = jnp.where(top, total[:, :128], total[:, 128:])
            if step:
                snd2[pl.ds(j, 1)] = tile[None]
                to_member(snd2.at[j], rcv2.at[me], sem_b, step).start()
            else:
                rcv2[pl.ds(me, 1)] = tile[None]
        for step in range(1, n_mem):
            to_member(
                snd2.at[lax.rem(me + step, n_mem)], rcv2.at[lax.rem(me + n_mem - step, n_mem)], sem_b, step
            ).wait()
        halves = ([], [])
        for v in range(q_all // 8):
            a, b = rcv2[2 * v], rcv2[2 * v + 1]
            halves[0].append(jnp.where(top, a, pltpu.roll(b, 4, 0)))
            halves[1].append(jnp.where(top, pltpu.roll(a, 4, 0), b))
        return [jnp.concatenate(half, axis=0) for half in halves]

    def make_image(halves):
        total = jnp.zeros((q_all, BLK), F32)
        for h in range(2):
            stack = []
            for s in range(4):
                stack += pieces(jnp.where(band == s, halves[h], 0.0))
            found = nn(jnp.concatenate(stack, axis=0), cst[h])
            for s in range(4):
                lifted = found[2 * s * q_all : (2 * s + 1) * q_all] + found[(2 * s + 1) * q_all : (2 * s + 2) * q_all]
                direction = d_ref[4 * h + s]
                image = nn((direction + lifted).astype(BF16), kmat[4 * h + s])
                img[4 * h + s] = image
                total = total + direction * image
        return total

    r_ref[...] = r_in[...]
    d_ref[...] = d_in[...]
    total = jnp.zeros((q_all, BLK), F32)
    for s in range(subs):
        total = total + r_ref[s] * nn(r_ref[s].astype(BF16), dmat[s])
    reduce_start(0, as_row(total))
    send_partials()
    reduce_middle(0)
    build_masks()
    invert_blocks()
    norm_start = reduce_end(0)

    def iteration(t, norm_now):
        scatter()
        coarse_solve(fold_neighbours())
        spread_neighbours()
        total = make_image(pick())
        curvature = all_reduce(1, as_row(total))
        alpha = norm_now / curvature
        steps_ref[pl.ds(t, 1), :] = alpha
        column = as_column(alpha)
        total = jnp.zeros((q_all, BLK), F32)
        for s in range(subs):
            residual = r_ref[s] - column * img[s]
            r_ref[s] = residual
            precond = nn(residual.astype(BF16), dmat[s])
            img[s] = precond
            total = total + residual * precond
        norm_next = all_reduce(0, as_row(total))
        column = as_column(norm_next / norm_now)
        for s in range(subs):
            d_ref[s] = img[s] + column * d_ref[s]

        @pl.when(t < ITERS - 1)
        def _():
            send_partials()

        return norm_next

    lax.fori_loop(0, ITERS, iteration, norm_start)


def local(n_grp, n_mem, residual, direction, local_inverse, dirichlet, coupling, corner_map, coarse_factor):
    subs, q_all, nr = residual.shape
    corners = coupling.shape[1]
    order = coarse_factor.shape[1]
    nb = order // BLK
    n_rows = 12 * nb
    cst = jnp.pad(coupling, ((0, 0), (0, 32 - corners), (0, 0))).reshape(2, 128, nr)
    idx = jnp.pad(corner_map, ((0, 0), (0, 32 - corners)), constant_values=-1).reshape(2, 1, 128)
    idx = jnp.broadcast_to(idx, (2, 4, 128)).reshape(8, 128)
    vmem = pl.BlockSpec(memory_space=pltpu.VMEM)
    dma = pltpu.SemaphoreType.DMA
    residual, direction, steps = pl.pallas_call(
        functools.partial(kernel, n_grp, n_mem),
        out_shape=(
            jax.ShapeDtypeStruct(residual.shape, F32),
            jax.ShapeDtypeStruct(residual.shape, F32),
            jax.ShapeDtypeStruct((8, 128), F32),
        ),
        in_specs=[vmem] * 6 + [pl.BlockSpec(memory_space=pl.ANY)],
        out_specs=(vmem,) * 3,
        scratch_shapes=[
            pltpu.VMEM((subs, q_all, nr), F32),
            pltpu.VMEM((order, order), BF16),
            pltpu.VMEM((nb, BLK, BLK), BF16),
            pltpu.VMEM((nb, BLK, BLK), BF16),
            pltpu.VMEM((BLK, n_mem * BLK), BF16),
            pltpu.VMEM((n_rows, n_mem * BLK), F32),
            pltpu.VMEM((2 * n_rows, n_mem * BLK), BF16),
            pltpu.VMEM((n_mem, 8, 128), F32),
            pltpu.VMEM((n_mem, 8, 128), F32),
            pltpu.VMEM((n_mem, 8, 128), F32),
            pltpu.VMEM((n_mem, 8, 128), F32),
            pltpu.VMEM((n_mem, 8, 128), jnp.int32),
            pltpu.VMEM((n_rows, BLK), F32),
            pltpu.VMEM((2, 4 * nb, BLK), F32),
            pltpu.VMEM((n_rows, BLK), F32),
            pltpu.VMEM((2, 2, max(n_mem, n_grp), 1, 128), F32),
            dma,
            dma((2, n_mem)),
            dma((2, n_mem)),
            dma((2, n_mem)),
            dma((2, n_grp)),
            dma((2, n_grp)),
            dma((2, 2, 2, max(n_mem, n_grp))),
        ],
        compiler_params=pltpu.CompilerParams(
            collective_id=0, has_side_effects=True, vmem_limit_bytes=64 * 1024 * 1024 - 512 * 1024
        ),
    )(residual, direction, local_inverse, dirichlet, cst, idx, coarse_factor)
    return residual, direction, steps[:ITERS, :q_all]


def solution(mesh):
    both = ("grp", "mem")
    return jax.shard_map(
        functools.partial(local, mesh.shape["grp"], mesh.shape["mem"]),
        mesh=mesh,
        in_specs=(P(both), P(both), P(both), P(both), P(both), P(both), P("grp")),
        out_specs=(P(both), P(both), P()),
        check_vma=False,
    )
```

```python
import functools

import jax
import jax.numpy as jnp
from jax import lax
from jax.experimental import pallas as pl
from jax.experimental.pallas import tpu as pltpu
from jax.sharding import PartitionSpec as P

ITERS = 3
MESH = pl.DeviceIdType.MESH
F32, BF16 = jnp.float32, jnp.bfloat16
BLK = 256


def nn(a, b):
    return lax.dot_general(a, b, (((1,), (0,)), ((), ())), preferred_element_type=F32)


def nt(a, b):
    return lax.dot_general(a, b, (((1,), (1,)), ((), ())), preferred_element_type=F32)


def pieces(x):
    high = x.astype(BF16)
    return high, (x - high.astype(F32)).astype(BF16)


def iota(shape, dim):
    return lax.broadcasted_iota(jnp.int32, shape, dim)


def kernel(
    n_grp, n_mem,
    r_in, d_in, kmat_in, dmat_in, coupling_in, corner_map, factor,
    r_ref, d_ref, steps_ref,
    kmat, dmat, coupling, cst, v_ref, solved, track, lift, l_ref, xh, xl, oht, mask, a_ref,
    idx, snd, rcv, snd2, rcv2, idx_all, load, nbr, ext, y_ref, ar,
    sem_l, sem_i, sem_f, sem_b, sem_n, sem_x, sem_a,
):
    subs, q_all, _ = r_in.shape
    corners = coupling_in.shape[1]
    nb = l_ref.shape[0] // BLK
    rows4 = 4 * nb
    n_rows = 3 * rows4
    me, grp = lax.axis_index("mem"), lax.axis_index("grp")
    top = iota((8, 128), 0) < 4
    top2 = iota((8, BLK), 0) < 4
    band = iota((q_all, 128), 1) // 32
    order = [0]
    for near in range(1, n_mem // 2):
        order += [near, n_mem - near]
    order.append(n_mem // 2)
    chunk = min(4, n_mem)

    barrier = pltpu.get_barrier_semaphore()
    for step in range(1, n_mem):
        pl.semaphore_signal(
            barrier, inc=1, device_id={"mem": lax.rem(me + step, n_mem)}, device_id_type=MESH
        )
    for step in range(1, n_grp):
        pl.semaphore_signal(
            barrier, inc=1, device_id={"grp": lax.rem(grp + step, n_grp)}, device_id_type=MESH
        )

    fetches = [
        pltpu.make_async_copy(src, dst, sem_l.at[number])
        for number, (src, dst) in enumerate(
            ((d_in, v_ref), (kmat_in, kmat), (coupling_in, coupling), (r_in, r_ref), (dmat_in, dmat), (factor.at[0], l_ref))
        )
    ]
    for fetch in fetches:
        fetch.start()

    def to_member(src, dst, sem, step):
        return pltpu.make_async_remote_copy(
            src_ref=src, dst_ref=dst, send_sem=sem.at[0, step], recv_sem=sem.at[1, step],
            device_id={"mem": lax.rem(me + step, n_mem)}, device_id_type=MESH,
        )

    def to_group(src, dst, sem, step):
        return pltpu.make_async_remote_copy(
            src_ref=src, dst_ref=dst, send_sem=sem.at[0, step], recv_sem=sem.at[1, step],
            device_id={"grp": lax.rem(grp + step, n_grp)}, device_id_type=MESH,
        )

    def member_at(step):
        return lax.rem(me + step, n_mem)

    def reduce_start(which, row):
        mine = ar.at[which, 0]
        mine[pl.ds(me, 1)] = row[None]
        for step in reversed(order[1:]):
            to_member(mine.at[me], mine.at[me], sem_a.at[which, 0], step).start()

    def reduce_middle(which):
        mine, other = ar.at[which, 0], ar.at[which, 1]
        for step in range(1, n_mem):
            to_member(mine.at[me], mine.at[member_at(n_mem - step)], sem_a.at[which, 0], step).wait()
        row = jnp.sum(mine[0:n_mem], axis=0)
        other[pl.ds(grp, 1)] = row[None]
        for step in range(1, n_grp):
            to_group(other.at[grp], other.at[grp], sem_a.at[which, 1], step).start()

    def reduce_end(which):
        other = ar.at[which, 1]
        for step in range(1, n_grp):
            to_group(other.at[grp], other.at[lax.rem(grp + n_grp - step, n_grp)], sem_a.at[which, 1], step).wait()
        return jnp.sum(other[0:n_grp], axis=0)

    def as_row(total):
        wide = jnp.concatenate([total, jnp.zeros((128 - q_all, BLK), F32)], axis=0)
        first, rest = wide.astype(BF16), wide
        ones = jnp.ones((8, BLK), BF16)
        rest = rest - first.astype(F32)
        second = rest.astype(BF16)
        third = (rest - second.astype(F32)).astype(BF16)
        out = nt(ones, first) + (nt(ones, second) + nt(ones, third))
        return out[0:1]

    def as_column(row):
        diagonal = iota((q_all, 128), 0) == iota((q_all, 128), 1)
        return jnp.sum(jnp.where(diagonal, jnp.broadcast_to(row, (q_all, 128)), 0.0), axis=1, keepdims=True)

    mine4 = iota((8, 128), 1) == 4 * me + lax.rem(iota((8, 128), 0), 4)

    def as_my_column(row):
        return jnp.sum(jnp.where(mine4, jnp.broadcast_to(row, (8, 128)), 0.0), axis=1, keepdims=True)

    def as_my_row(column):
        return jnp.sum(jnp.where(mine4 & top, jnp.broadcast_to(column, (8, 128)), 0.0), axis=0, keepdims=True)

    def build_tables():
        cst[...] = jnp.zeros(cst.shape, BF16)
        for s in range(subs):
            cst[s // 4, 32 * (s % 4) : 32 * (s % 4) + corners, :] = coupling[s]
        idx[...] = jnp.full((8, 128), -1, jnp.int32)
        idx[:, 0:corners] = corner_map[...]
        wide = idx[...]
        lane, sub = iota((8, 128), 1) // 32, iota((8, 128), 0)
        tile = jnp.full((8, 128), -1, jnp.int32)
        for s in range(subs):
            turned = pltpu.roll(wide, 32 * (s % 4), 1)[s : s + 1] if s % 4 else wide[s : s + 1]
            tile = jnp.where((lane == s % 4) & (sub // 4 == s // 4), jnp.broadcast_to(turned, (8, 128)), tile)
        idx[...] = tile

    def local_partials():
        halves = []
        for h in range(2):
            stack = []
            for s in range(4 * h, 4 * h + 4):
                out = nn(v_ref[s].astype(BF16), kmat[s])
                solved[s] = out
                stack += pieces(out)
            found = nt(jnp.concatenate(stack, axis=0), cst[h])
            total = jnp.zeros((q_all, 128), F32)
            for s in range(4):
                part = found[2 * s * q_all : (2 * s + 1) * q_all] + found[(2 * s + 1) * q_all : (2 * s + 2) * q_all]
                total = jnp.where(band == s, part, total)
            halves.append(total)
        for v in range(q_all // 8):
            a, b = halves[0][8 * v : 8 * v + 8], halves[1][8 * v : 8 * v + 8]
            snd[2 * v] = jnp.where(top, a, pltpu.roll(b, 4, 0))
            snd[2 * v + 1] = jnp.where(top, pltpu.roll(a, 4, 0), b)

    def send_partials():
        for step in reversed(order[1:]):
            to_member(snd.at[member_at(step)], rcv.at[me], sem_f, step).start()
        rcv[pl.ds(me, 1)] = snd[pl.ds(me, 1)]

    def block(i, j):
        return l_ref[i * BLK : (i + 1) * BLK, j * BLK : (j + 1) * BLK]

    def triple(left, high, low):
        left_high, left_low = pieces(left)
        return nn(left_high, high) + (nn(left_high, low) + nn(left_low, high))

    def invert_blocks(first, count):
        row, col = iota((BLK, BLK), 0), iota((BLK, BLK), 1)
        inverses = []
        for i in range(first, first + count):
            tri = block(i, i).astype(F32)
            diag = jnp.where(row == col, tri, 0.0)
            down = 1.0 / jnp.sum(diag, axis=1, keepdims=True)
            across = 1.0 / jnp.sum(diag, axis=0, keepdims=True)
            below = (row // 2 == col // 2) & (row > col)
            inverses.append(jnp.where(row == col, down, 0.0) - jnp.where(below, tri * down * across, 0.0))
        size = 2
        while size < BLK // 2:
            below = (row // (2 * size) == col // (2 * size)) & (row // size > col // size)
            split = [pieces(inv) for inv in inverses]
            lefts = []
            for number, (high, low) in enumerate(split):
                off = jnp.where(below, block(first + number, first + number).astype(F32), 0.0).astype(BF16)
                lefts.append(nn(high, off) + nn(low, off))
            inverses = [inv - triple(left, *pair) for inv, left, pair in zip(inverses, lefts, split)]
            size *= 2
        half = BLK // 2
        for number, inv in enumerate(inverses):
            i = first + number
            high, low = pieces(inv)
            xh[i // 2, i % 2] = high
            xl[i // 2, i % 2] = low
            off = l_ref[i * BLK + half : (i + 1) * BLK, i * BLK : i * BLK + half]
            left = nn(high[half:, half:], off) + nn(low[half:, half:], off)
            high, low = pieces(-triple(left, high[:half, :half], low[:half, :half]))
            xh[i // 2, i % 2, half:, :half] = high
            xl[i // 2, i % 2, half:, :half] = low
        for u in range(first // 2, (first + count) // 2):
            off = block(2 * u + 1, 2 * u)
            left = nn(xh[u, 1], off) + nn(xl[u, 1], off)
            xh[u, 2], xl[u, 2] = pieces(-triple(left, xh[u, 0], xl[u, 0]))

    def build_masks():
        for step in range(1, n_mem):
            to_member(idx, idx_all.at[member_at(n_mem - step)], sem_i, step).wait()
        for position, step in enumerate(order):
            tile = idx_all[pl.ds(member_at(n_mem - step), 1)][0]
            for h in range(2):
                line = tile[4 * h : 4 * h + 1]
                at = position * BLK + h * 128
                lo = jnp.broadcast_to(line & (BLK - 1), (BLK, 128))
                oht[:, at : at + 128] = jnp.where(lo == iota((BLK, 128), 0), 1.0, 0.0).astype(BF16)
                hi = jnp.broadcast_to(line >> 8, (n_rows, 128))
                mask[:, at : at + 128] = jnp.where(hi == iota((n_rows, 128), 0) // 4, 1.0, 0.0)

    def scatter():
        total = jnp.zeros((2 * n_rows, BLK), F32)
        for position, step in enumerate(order):
            j = member_at(n_mem - step)
            if step:
                to_member(snd.at[member_at(step)], rcv.at[j], sem_f, step).wait()
            tile = rcv[pl.ds(j, 1)][0]
            high = tile.astype(BF16).astype(F32)
            for number, part in enumerate((high, tile - high)):
                turned = pltpu.roll(part, 4, 0)
                for h in range(2):
                    twice = jnp.where(top, part, turned) if h == 0 else jnp.where(top, turned, part)
                    at = position * BLK + h * 128
                    full = jnp.concatenate([twice] * (n_rows // 8), axis=0) * mask[:, at : at + 128]
                    a_ref[number * n_rows : (number + 1) * n_rows, at : at + 128] = full.astype(BF16)
            if position % chunk == chunk - 1:
                at = slice((position + 1 - chunk) * BLK, (position + 1) * BLK)
                total = total + nt(a_ref[:, at], oht[:, at])
        load[...] = total[:n_rows] + total[n_rows:]

    def twin(x):
        high, low = pieces(x)
        return jnp.where(top2, high.astype(F32), low.astype(F32)).astype(BF16)

    def folded(x):
        return x + pltpu.roll(x, 4, 0)

    def lower(b):
        acc = []
        for v in range(nb // 2):
            x = b[8 * v : 8 * v + 8]
            y = pltpu.roll(x, 4, 0)
            acc += [jnp.where(top2, x, y), jnp.where(top2, y, x)]
        for u in range(nb // 2):
            p0, p1 = twin(acc[2 * u]), twin(acc[2 * u + 1])
            y0 = nt(p0, xh[u, 0]) + nt(p0, xl[u, 0])
            y1 = (nt(p0, xh[u, 2]) + nt(p0, xl[u, 2])) + (nt(p1, xh[u, 1]) + nt(p1, xl[u, 1]))
            acc[2 * u], acc[2 * u + 1] = folded(y0), folded(y1)
            p0, p1 = twin(acc[2 * u]), twin(acc[2 * u + 1])
            for t in range(2 * u + 2, nb):
                acc[t] = acc[t] - folded(nt(p0, block(t, 2 * u)) + nt(p1, block(t, 2 * u + 1)))
        return acc

    def upper(acc):
        for u in reversed(range(nb // 2)):
            p0, p1 = twin(acc[2 * u]), twin(acc[2 * u + 1])
            x1 = nn(p1, xh[u, 1]) + nn(p1, xl[u, 1])
            x0 = (nn(p0, xh[u, 0]) + nn(p0, xl[u, 0])) + (nn(p1, xh[u, 2]) + nn(p1, xl[u, 2]))
            acc[2 * u], acc[2 * u + 1] = folded(x0), folded(x1)
            p0, p1 = twin(acc[2 * u]), twin(acc[2 * u + 1])
            for t in range(2 * u):
                acc[t] = acc[t] - folded(nn(p0, block(2 * u, t)) + nn(p1, block(2 * u + 1, t)))
        for v in range(nb // 2):
            ext[rows4 + 8 * v : rows4 + 8 * v + 8] = jnp.where(top2, acc[2 * v], acc[2 * v + 1])

    def pick():
        high, low = pieces(ext[...])
        both = jnp.concatenate([high, low], axis=0)
        for position in reversed(range(n_mem)):
            step = (n_mem - order[position]) % n_mem
            j = member_at(step)
            at = slice(position * BLK, (position + 1) * BLK)
            found = nn(both, oht[:, at])
            found = (found[:n_rows] + found[n_rows:]) * mask[:, at]
            total = found[0:8]
            for v in range(1, n_rows // 8):
                total = total + found[8 * v : 8 * v + 8]
            total = folded(total)
            tile = jnp.where(top, total[:, :128], total[:, 128:])
            if step:
                snd2[pl.ds(j, 1)] = tile[None]
                to_member(snd2.at[j], rcv2.at[me], sem_b, step).start()
            else:
                rcv2[pl.ds(me, 1)] = tile[None]

    def picked():
        for step in order[1:]:
            to_member(snd2.at[member_at(step)], rcv2.at[member_at(n_mem - step)], sem_b, step).wait()
        halves = ([], [])
        for v in range(q_all // 8):
            a, b = rcv2[2 * v], rcv2[2 * v + 1]
            halves[0].append(jnp.where(top, a, pltpu.roll(b, 4, 0)))
            halves[1].append(jnp.where(top, pltpu.roll(a, 4, 0), b))
        return [jnp.concatenate(half, axis=0) for half in halves]

    def update(halves, alpha, beta):
        total = jnp.zeros((q_all, BLK), F32)
        for h in range(2):
            stack = []
            for s in range(4):
                stack += pieces(jnp.where(band == s, halves[h], 0.0))
            found = nn(jnp.concatenate(stack, axis=0), cst[h])
            for s in range(4):
                lifted = found[2 * s * q_all : (2 * s + 1) * q_all] + found[(2 * s + 1) * q_all : (2 * s + 2) * q_all]
                at = 4 * h + s
                lifted = lifted + beta * lift[at]
                lift[at] = lifted
                image = nn((d_ref[at] + lifted).astype(BF16), kmat[at])
                residual = r_ref[at] - alpha * image
                r_ref[at] = residual
                precond = nn(residual.astype(BF16), dmat[at])
                v_ref[at] = precond
                total = total + residual * precond
        return total

    d_ref[...] = jnp.zeros(d_ref.shape, F32)
    track[...] = jnp.zeros(track.shape, F32)
    lift[...] = jnp.zeros(lift.shape, F32)
    y_ref[...] = jnp.zeros(y_ref.shape, F32)
    for fetch in fetches[:3]:
        fetch.wait()
    build_tables()
    local_partials()
    for fetch in fetches[3:5]:
        fetch.wait()
    total = jnp.zeros((q_all, BLK), F32)
    for s in range(subs):
        total = total + r_ref[s] * nn(r_ref[s].astype(BF16), dmat[s])
    first_row = as_row(total)
    pl.semaphore_wait(barrier, n_mem + n_grp - 2)
    reduce_start(0, first_row)
    send_partials()
    idx_all[pl.ds(me, 1)] = idx[...][None]
    for step in reversed(order[1:]):
        to_member(idx, idx_all.at[me], sem_i, step).start()
    fetches[5].wait()
    group = min(4, nb)
    invert_blocks(0, group)
    build_masks()
    for start in range(group, nb, group):
        invert_blocks(start, group)

    def iteration(t, norm_before):
        reduce_middle(0)
        scatter()
        up = to_group(load.at[2 * rows4 : 3 * rows4], nbr.at[0], sem_n, 1)
        down = to_group(load.at[0:rows4], nbr.at[1], sem_n, n_grp - 1)
        up.start()
        down.start()
        norm_now = reduce_end(0)
        beta = jnp.where(t == 0, 0.0, norm_now / norm_before)
        beta_column = as_column(beta)
        total = jnp.zeros((q_all, BLK), F32)
        for s in range(subs):
            direction = v_ref[s] + beta_column * d_ref[s]
            d_ref[s] = direction
            follow = solved[s] + beta_column * track[s]
            track[s] = follow
            total = total + direction * follow
        local_row = as_row(total)
        up.wait()
        down.wait()
        acc = lower(load[rows4 : 2 * rows4] + nbr[0] + nbr[1])
        my_beta = as_my_column(beta)
        squares = jnp.zeros((8, BLK), F32)
        for i in range(nb):
            y = acc[i] + my_beta * y_ref[i]
            y_ref[i] = y
            squares = squares + y * y
        reduce_start(1, local_row + as_my_row(jnp.sum(squares, axis=1, keepdims=True)))
        upper(acc)
        own = ext.at[rows4 : 2 * rows4]
        up = to_group(own, ext.at[0:rows4], sem_x, 1)
        down = to_group(own, ext.at[2 * rows4 : 3 * rows4], sem_x, n_grp - 1)
        up.start()
        down.start()
        reduce_middle(1)
        up.wait()
        down.wait()
        pick()
        alpha = norm_now / reduce_end(1)
        steps_ref[pl.ds(t, 1), :] = alpha[:, :q_all]
        reduce_start(0, as_row(update(picked(), as_column(alpha), beta_column)))

        @pl.when(t < ITERS - 1)
        def _():
            local_partials()
            send_partials()

        return norm_now

    norm_before = lax.fori_loop(0, ITERS, iteration, jnp.ones((1, 128), F32))
    reduce_middle(0)
    beta_column = as_column(reduce_end(0) / norm_before)
    for s in range(subs):
        d_ref[s] = v_ref[s] + beta_column * d_ref[s]


def local(n_grp, n_mem, residual, direction, local_inverse, dirichlet, coupling, corner_map, coarse_factor):
    subs, q_all, nr = residual.shape
    order = coarse_factor.shape[1]
    nb = order // BLK
    n_rows = 12 * nb
    most = max(n_mem, n_grp)
    dma = pltpu.SemaphoreType.DMA
    vmem = pl.BlockSpec(memory_space=pltpu.VMEM)
    anywhere = pl.BlockSpec(memory_space=pl.ANY)
    field = pltpu.VMEM(residual.shape, F32)
    tiles = pltpu.VMEM((n_mem, 8, 128), F32)
    return pl.pallas_call(
        functools.partial(kernel, n_grp, n_mem),
        out_shape=(
            jax.ShapeDtypeStruct(residual.shape, F32),
            jax.ShapeDtypeStruct(residual.shape, F32),
            jax.ShapeDtypeStruct((ITERS, q_all), F32),
        ),
        in_specs=[anywhere] * 5 + [vmem, anywhere],
        out_specs=(vmem,) * 3,
        scratch_shapes=[
            pltpu.VMEM(local_inverse.shape, BF16),
            pltpu.VMEM(dirichlet.shape, BF16),
            pltpu.VMEM(coupling.shape, BF16),
            pltpu.VMEM((2, 128, nr), BF16),
            field,
            field,
            field,
            field,
            pltpu.VMEM((order, order), BF16),
            pltpu.VMEM((nb // 2, 3, BLK, BLK), BF16),
            pltpu.VMEM((nb // 2, 3, BLK, BLK), BF16),
            pltpu.VMEM((BLK, n_mem * BLK), BF16),
            pltpu.VMEM((n_rows, n_mem * BLK), F32),
            pltpu.VMEM((2 * n_rows, n_mem * BLK), BF16),
            pltpu.VMEM((8, 128), jnp.int32),
            tiles,
            tiles,
            tiles,
            tiles,
            pltpu.VMEM((n_mem, 8, 128), jnp.int32),
            pltpu.VMEM((n_rows, BLK), F32),
            pltpu.VMEM((2, 4 * nb, BLK), F32),
            pltpu.VMEM((n_rows, BLK), F32),
            pltpu.VMEM((nb, 8, BLK), F32),
            pltpu.VMEM((2, 2, most, 1, 128), F32),
            dma((6,)),
            dma((2, n_mem)),
            dma((2, n_mem)),
            dma((2, n_mem)),
            dma((2, n_grp)),
            dma((2, n_grp)),
            dma((2, 2, 2, most)),
        ],
        compiler_params=pltpu.CompilerParams(
            collective_id=0, has_side_effects=True, vmem_limit_bytes=63 * 1024 * 1024
        ),
    )(residual, direction, local_inverse, dirichlet, coupling, corner_map, coarse_factor)


def solution(mesh):
    both = ("grp", "mem")
    return jax.shard_map(
        functools.partial(local, mesh.shape["grp"], mesh.shape["mem"]),
        mesh=mesh,
        in_specs=(P(both), P(both), P(both), P(both), P(both), P(both), P("grp")),
        out_specs=(P(both), P(both), P()),
        check_vma=False,
    )
```

```python
import functools

import jax
import jax.numpy as jnp
from jax import lax
from jax.experimental import pallas as pl
from jax.experimental.pallas import tpu as pltpu
from jax.sharding import PartitionSpec as P

ITERS = 3
MESH = pl.DeviceIdType.MESH
F32, BF16 = jnp.float32, jnp.bfloat16
BLK = 256
VMEM_LIMIT = 63 * 1024 * 1024


def nn(a, b):
    return lax.dot_general(a, b, (((1,), (0,)), ((), ())), preferred_element_type=F32)


def nt(a, b):
    return lax.dot_general(a, b, (((1,), (1,)), ((), ())), preferred_element_type=F32)


def pieces(x):
    high = x.astype(BF16)
    return high, (x - high.astype(F32)).astype(BF16)


def iota(shape, dim):
    return lax.broadcasted_iota(jnp.int32, shape, dim)


def kernel(
    n_grp, n_mem,
    r_in, d_in, kmat_in, dmat_in, coupling_in, corner_map, factor,
    r_out, v_out, d_out, rows_ref,
    r_ref, v_ref, d_ref, kmat, dmat, coupling, cst, solved, track, lift, l_ref, xh, xl, oht, mask, a_ref,
    idx, snd, rcv, snd2, rcv2, idx_all, load, nbr, ext, sums, y_new, y_old, ar, energy,
    sem_l, sem_o, sem_i, sem_f, sem_b, sem_n, sem_x, sem_a, sem_e,
):
    subs, q_all, _ = r_in.shape
    corners = coupling_in.shape[1]
    nb = l_ref.shape[0] // BLK
    rows4 = 4 * nb
    n_rows = 3 * rows4
    me, grp = lax.axis_index("mem"), lax.axis_index("grp")
    top = iota((8, 128), 0) < 4
    top2 = iota((8, BLK), 0) < 4
    band = iota((q_all, 128), 1) // 32
    order = [0]
    for near in range(1, n_mem // 2):
        order += [near, n_mem - near]
    order.append(n_mem // 2)
    chunk = min(4, n_mem)
    n_chunks = n_mem // chunk
    even = lax.rem(grp, 2) == 0
    near_step = jnp.where(even, 1, n_grp - 1)
    far_step = jnp.where(even, n_grp - 1, 1)

    def span(u, count):
        return pl.ds(2 * BLK * u, 2 * BLK * count)

    side = lax.rem(grp // 2, 2)
    across = me + 1 - 2 * lax.rem(me, 2)

    def member_at(step):
        return lax.rem(me + step, n_mem)

    def flip(member):
        return member + side * (1 - 2 * lax.rem(member, 2))

    mine = flip(me)

    def same_rows(step):
        other = lax.rem(grp + step, n_grp)
        turn = lax.rem(other // 2, 2) - side
        return {"grp": other, "mem": me + turn * turn * (1 - 2 * lax.rem(me, 2))}

    barrier = pltpu.get_barrier_semaphore()
    for step in range(1, n_mem):
        pl.semaphore_signal(barrier, inc=1, device_id={"mem": member_at(step)}, device_id_type=MESH)
    for step in range(1, n_grp):
        pl.semaphore_signal(barrier, inc=1, device_id=same_rows(step), device_id_type=MESH)

    fetches = [
        pltpu.make_async_copy(src, dst, sem_l.at[number])
        for number, (src, dst) in enumerate(
            [(d_in, v_ref), (kmat_in, kmat), (coupling_in, coupling), (r_in, r_ref), (dmat_in, dmat)]
            + [(factor.at[0, span(u, 1), span(u, 1)], l_ref.at[span(u, 1), span(u, 1)]) for u in range(nb // 2)]
            + [
                (factor.at[0, span(u + 1, nb // 2 - u - 1), span(u, 1)], l_ref.at[span(u + 1, nb // 2 - u - 1), span(u, 1)])
                for u in range(nb // 2 - 1)
            ]
        )
    ]
    for fetch in fetches:
        fetch.start()

    def to_member(src, dst, sem, step):
        return pltpu.make_async_remote_copy(
            src_ref=src, dst_ref=dst, send_sem=sem.at[0, step], recv_sem=sem.at[1, step],
            device_id={"mem": lax.rem(me + step, n_mem)}, device_id_type=MESH,
        )

    def to_group(src, dst, sem, step):
        return pltpu.make_async_remote_copy(
            src_ref=src, dst_ref=dst, send_sem=sem.at[0, step], recv_sem=sem.at[1, step],
            device_id=same_rows(step), device_id_type=MESH,
        )

    def to_neighbour(src, dst, sem, number, step, member):
        return pltpu.make_async_remote_copy(
            src_ref=src, dst_ref=dst, send_sem=sem.at[0, number], recv_sem=sem.at[1, number],
            device_id={"grp": lax.rem(grp + step, n_grp), "mem": member}, device_id_type=MESH,
        )

    def near_load():
        return to_neighbour(load.at[0:rows4], nbr.at[0], sem_n, nb // 2, near_step, me)

    def far_load(u):
        piece = pl.ds(8 * u, 8)
        return to_neighbour(load.at[pl.ds(2 * rows4 + 8 * u, 8)], nbr.at[1, piece], sem_n, u, far_step, across)

    def near_spread():
        return to_neighbour(ext.at[rows4 : 2 * rows4], ext.at[0:rows4], sem_x, nb // 2, near_step, me)

    def far_spread(u):
        return to_neighbour(
            ext.at[pl.ds(rows4 + 8 * u, 8)], ext.at[pl.ds(2 * rows4 + 8 * u, 8)], sem_x, u, far_step, across
        )

    def reduce_start(*rows):
        first = ar.at[0]
        for number, row in enumerate(rows):
            first[pl.ds(me, 1), number : number + 1, :] = row[None]
        for step in reversed(order[1:]):
            to_member(first.at[me], first.at[me], sem_a.at[0], step).start()

    def reduce_middle():
        first, second = ar.at[0], ar.at[1]
        for step in range(1, n_mem):
            to_member(first.at[me], first.at[member_at(n_mem - step)], sem_a.at[0], step).wait()
        second[pl.ds(grp, 1)] = jnp.sum(first[0:n_mem], axis=0)[None]
        for step in range(1, n_grp):
            to_group(second.at[grp], second.at[grp], sem_a.at[1], step).start()

    def reduce_end():
        second = ar.at[1]
        for step in range(1, n_grp):
            to_group(second.at[grp], second.at[lax.rem(grp + n_grp - step, n_grp)], sem_a.at[1], step).wait()
        return jnp.sum(second[0:n_grp], axis=0)

    def energy_start(squares, crosses):
        place = iota((8, 128), 0) == iota((8, 128), 1)
        column = jnp.where(top, jnp.broadcast_to(squares, (8, 128)), jnp.broadcast_to(crosses, (8, 128)))
        energy[pl.ds(grp, 1)] = jnp.sum(jnp.where(place, column, 0.0), axis=0, keepdims=True)[None]
        for step in range(1, n_grp):
            to_group(energy.at[grp], energy.at[grp], sem_e, step).start()

    def energy_end():
        for step in range(1, n_grp):
            to_group(energy.at[grp], energy.at[lax.rem(grp + n_grp - step, n_grp)], sem_e, step).wait()
        row = jnp.sum(energy[...], axis=0)
        place = iota((8, 128), 0) == iota((8, 128), 1)
        column = jnp.sum(jnp.where(place, jnp.broadcast_to(row, (8, 128)), 0.0), axis=1, keepdims=True)
        column = jnp.broadcast_to(column, (8, 128))
        return jnp.where(iota((8, 128), 1) == corners, column, pltpu.roll(column, 4, 0))

    def as_row(*totals):
        spare = 128 - q_all * len(totals)
        fill = [jnp.zeros((spare, BLK), F32)] if spare else []
        wide = jnp.concatenate([*totals, *fill], axis=0)
        first = wide.astype(BF16)
        rest = wide - first.astype(F32)
        second = rest.astype(BF16)
        third = (rest - second.astype(F32)).astype(BF16)
        ones = jnp.ones((8, BLK), BF16)
        out = nt(ones, first) + (nt(ones, second) + nt(ones, third))
        return out[0:1]

    def as_column(row, offset=0):
        diagonal = iota((q_all, 128), 0) + offset == iota((q_all, 128), 1)
        return jnp.sum(jnp.where(diagonal, jnp.broadcast_to(row, (q_all, 128)), 0.0), axis=1, keepdims=True)

    def back_to_row(column):
        diagonal = iota((q_all, 128), 0) == iota((q_all, 128), 1)
        return jnp.sum(jnp.where(diagonal, jnp.broadcast_to(column, (q_all, 128)), 0.0), axis=0, keepdims=True)

    mine4 = iota((8, 128), 1) == 4 * mine + lax.rem(iota((8, 128), 0), 4)

    def as_my_column(row):
        return jnp.sum(jnp.where(mine4, jnp.broadcast_to(row, (8, 128)), 0.0), axis=1, keepdims=True)

    def build_tables():
        cst[...] = jnp.zeros(cst.shape, BF16)
        for s in range(subs):
            cst[s // 4, 32 * (s % 4) : 32 * (s % 4) + corners, :] = coupling[s]
        idx[...] = jnp.full((8, 128), -1, jnp.int32)
        idx[:, 0:corners] = corner_map[...]
        wide = idx[...]
        lane, sub = iota((8, 128), 1) // 32, iota((8, 128), 0)
        tile = jnp.full((8, 128), -1, jnp.int32)
        for s in range(subs):
            turned = pltpu.roll(wide, 32 * (s % 4), 1)[s : s + 1] if s % 4 else wide[s : s + 1]
            tile = jnp.where((lane == s % 4) & (sub // 4 == s // 4), jnp.broadcast_to(turned, (8, 128)), tile)
        idx[...] = tile

    def local_partials():
        halves = []
        for h in range(2):
            stack = []
            for s in range(4 * h, 4 * h + 4):
                out = nn(v_ref[s].astype(BF16), kmat[s])
                solved[s] = out
                stack += pieces(out)
            found = nt(jnp.concatenate(stack, axis=0), cst[h])
            total = jnp.zeros((q_all, 128), F32)
            for s in range(4):
                part = found[2 * s * q_all : (2 * s + 1) * q_all] + found[(2 * s + 1) * q_all : (2 * s + 2) * q_all]
                total = jnp.where(band == s, part, total)
            halves.append(total)
        for v in range(q_all // 8):
            a, b = halves[0][8 * v : 8 * v + 8], halves[1][8 * v : 8 * v + 8]
            snd[2 * v] = jnp.where(top, a, pltpu.roll(b, 4, 0))
            snd[2 * v + 1] = jnp.where(top, pltpu.roll(a, 4, 0), b)

    def send_partials():
        for step in reversed(order[1:]):
            to_member(snd.at[flip(member_at(step))], rcv.at[me], sem_f, step).start()
        rcv[pl.ds(me, 1)] = snd[pl.ds(mine, 1)]

    def block(i, j):
        return l_ref[i * BLK : (i + 1) * BLK, j * BLK : (j + 1) * BLK]

    def triple(left, high, low):
        left_high, left_low = pieces(left)
        return nn(left_high, high) + (nn(left_high, low) + nn(left_low, high))

    half = BLK // 2

    def between(high, low, off, high_after, low_after):
        left = nn(jnp.concatenate([high, low], axis=1), jnp.concatenate([off, off], axis=0))
        left = jnp.concatenate(pieces(left), axis=1)
        after = jnp.concatenate(
            [
                jnp.concatenate([high_after, low_after], axis=1),
                jnp.concatenate([high_after, jnp.zeros_like(low_after)], axis=1),
            ],
            axis=0,
        )
        out = nn(left, after)
        return out[:, :half] + out[:, half:]

    def invert_blocks(first, count):
        row, col = iota((half, half), 0), iota((half, half), 1)
        numbers = range(2 * first, 2 * (first + count))

        def tile(i, j):
            return l_ref[i * half : (i + 1) * half, j * half : (j + 1) * half]

        inverses = []
        for i in numbers:
            tri = tile(i, i).astype(F32)
            diag = jnp.where(row == col, tri, 0.0)
            down = 1.0 / jnp.sum(diag, axis=1, keepdims=True)
            along = 1.0 / jnp.sum(diag, axis=0, keepdims=True)
            below = (row // 2 == col // 2) & (row > col)
            inverses.append(jnp.where(row == col, down, 0.0) - jnp.where(below, tri * down * along, 0.0))
        size = 2
        while size < half:
            below = (row // (2 * size) == col // (2 * size)) & (row // size > col // size)
            split = [pieces(inv) for inv in inverses]
            offs = [jnp.where(below, tile(i, i).astype(F32), 0.0).astype(BF16) for i in numbers]
            inverses = [
                inv - between(*pair, off, *pair) for inv, pair, off in zip(inverses, split, offs)
            ]
            size *= 2
        split = [pieces(inv) for inv in inverses]
        nothing = jnp.zeros((half, half), BF16)
        for number in range(count):
            i = first + number
            before, after = split[2 * number], split[2 * number + 1]
            corner = pieces(-between(*after, tile(2 * i + 1, 2 * i), *before))
            for ref, a, b, c in zip((xh, xl), before, after, corner):
                ref[i // 2, i % 2, :half, :half] = a
                ref[i // 2, i % 2, :half, half:] = nothing
                ref[i // 2, i % 2, half:, :half] = c
                ref[i // 2, i % 2, half:, half:] = b
        for u in range(first // 2, (first + count) // 2):
            off = block(2 * u + 1, 2 * u)
            left = nn(xh[u, 1], off) + nn(xl[u, 1], off)
            xh[u, 2], xl[u, 2] = pieces(-triple(left, xh[u, 0], xl[u, 0]))

    def build_masks():
        for step in range(1, n_mem):
            to_member(idx, idx_all.at[member_at(n_mem - step)], sem_i, step).wait()
        for position, step in enumerate(order):
            tile = idx_all[pl.ds(member_at(n_mem - step), 1)][0]
            for h in range(2):
                line = tile[4 * h : 4 * h + 1]
                at = position * BLK + h * 128
                lo = jnp.broadcast_to(line & (BLK - 1), (BLK, 128))
                oht[:, at : at + 128] = jnp.where(lo == iota((BLK, 128), 0), 1.0, 0.0).astype(BF16)
                below, above = jnp.where(even, 2 * nb, 0), jnp.where(even, 0, 2 * nb)
                hi = line >> 8
                moved = jnp.where(hi < nb, hi + below, jnp.where(hi < 2 * nb, hi, hi - 2 * nb + above))
                hi = jnp.broadcast_to(jnp.where(hi < 0, -1, moved), (n_rows, 128))
                mask[:, at : at + 128] = jnp.where(hi == iota((n_rows, 128), 0) // 4, 1.0, 0.0)

    def gather_chunk(number):
        positions = range(number * chunk, (number + 1) * chunk)
        for position in positions:
            step = order[position]
            if step:
                to_member(snd.at[flip(member_at(step))], rcv.at[member_at(n_mem - step)], sem_f, step).wait()
        for position in positions:
            tile = rcv[pl.ds(member_at(n_mem - order[position]), 1)][0]
            high = tile.astype(BF16).astype(F32)
            for number_of, part in enumerate((high, tile - high)):
                turned = pltpu.roll(part, 4, 0)
                for h in range(2):
                    twice = jnp.where(top, part, turned) if h == 0 else jnp.where(top, turned, part)
                    at = position * BLK + h * 128
                    full = jnp.concatenate([twice] * (n_rows // 8), axis=0) * mask[:, at : at + 128]
                    a_ref[number_of * n_rows : (number_of + 1) * n_rows, at : at + 128] = full.astype(BF16)
        at = slice(number * chunk * BLK, (number + 1) * chunk * BLK)
        total = nt(a_ref[:, at], oht[:, at])
        total = total[:n_rows] + total[n_rows:]
        load[...] = total if number == 0 else load[...] + total

    def twin(x):
        high, low = pieces(x)
        return jnp.where(top2, high.astype(F32), low.astype(F32)).astype(BF16)

    def folded(x):
        return x + pltpu.roll(x, 4, 0)

    def lower():
        acc, taken = [], [None] * nb
        near_load().wait()
        for u in range(nb // 2):
            far_load(u).wait()
            piece = slice(8 * u, 8 * u + 8)
            x = load[rows4 + 8 * u : rows4 + 8 * u + 8] + nbr[0, piece] + nbr[1, piece]
            y = pltpu.roll(x, 4, 0)
            b0, b1 = jnp.where(top2, x, y), jnp.where(top2, y, x)
            if u:
                b0, b1 = b0 - folded(taken[2 * u]), b1 - folded(taken[2 * u + 1])
            p0, p1 = twin(b0), twin(b1)
            y0 = nt(p0, xh[u, 0]) + nt(p0, xl[u, 0])
            y1 = (nt(p0, xh[u, 2]) + nt(p0, xl[u, 2])) + (nt(p1, xh[u, 1]) + nt(p1, xl[u, 1]))
            acc += [folded(y0), folded(y1)]
            p0, p1 = twin(acc[2 * u]), twin(acc[2 * u + 1])
            for t in range(2 * u + 2, nb):
                part = nt(p0, block(t, 2 * u)) + nt(p1, block(t, 2 * u + 1))
                taken[t] = part if taken[t] is None else taken[t] + part
        return acc

    def upper(acc):
        acc = list(acc)
        for u in reversed(range(nb // 2)):
            p0, p1 = twin(acc[2 * u]), twin(acc[2 * u + 1])
            x1 = nn(p1, xh[u, 1]) + nn(p1, xl[u, 1])
            x0 = (nn(p0, xh[u, 0]) + nn(p0, xl[u, 0])) + (nn(p1, xh[u, 2]) + nn(p1, xl[u, 2]))
            x0, x1 = folded(x0), folded(x1)
            ext[rows4 + 8 * u : rows4 + 8 * u + 8] = jnp.where(top2, x0, x1)
            far_spread(u).start()
            p0, p1 = twin(x0), twin(x1)
            for t in range(2 * u):
                acc[t] = acc[t] - folded(nn(p0, block(2 * u, t)) + nn(p1, block(2 * u + 1, t)))
        near_spread().start()

    def pick_rows(role, number):
        rows = slice(role * rows4, (role + 1) * rows4)
        at = slice(number * chunk * BLK, (number + 1) * chunk * BLK)
        high, low = pieces(ext[rows])
        found = nn(jnp.concatenate([high, low], axis=0), oht[:, at])
        found = (found[:rows4] + found[rows4:]) * mask[rows, at]
        total = found[0:8]
        for v in range(1, rows4 // 8):
            total = total + found[8 * v : 8 * v + 8]
        return total

    def pick_early():
        for number in range(n_chunks):
            sums[:, number * chunk * BLK : (number + 1) * chunk * BLK] = pick_rows(1, number)
        near_spread().wait()
        for number in range(n_chunks):
            at = slice(number * chunk * BLK, (number + 1) * chunk * BLK)
            sums[:, at] = sums[:, at] + pick_rows(0, number)

    def pick_chunk(number, extra):
        at = slice(number * chunk * BLK, (number + 1) * chunk * BLK)
        total = sums[:, at] + pick_rows(2, number)
        total = total + pltpu.roll(total, 4, 0)
        steps = []
        padding = top & (iota((8, 128), 1) // 2 == corners // 2)
        for position in range(chunk):
            step = (n_mem - order[number * chunk + position]) % n_mem
            begin = position * BLK
            tile = jnp.where(top, total[:, begin : begin + 128], total[:, begin + 128 : begin + 256])
            tile = jnp.where(padding, extra, tile)
            if step:
                snd2[pl.ds(member_at(step), 1)] = tile[None]
                steps.append(step)
            else:
                rcv2[pl.ds(mine, 1)] = tile[None]
        for step in reversed(steps):
            to_member(snd2.at[member_at(step)], rcv2.at[mine], sem_b, step).start()

    def picked():
        for step in order[1:]:
            to_member(snd2.at[member_at(step)], rcv2.at[flip(member_at(n_mem - step))], sem_b, step).wait()
        halves = ([], [])
        for v in range(q_all // 8):
            a, b = rcv2[2 * v], rcv2[2 * v + 1]
            halves[0].append(jnp.where(top, a, pltpu.roll(b, 4, 0)))
            halves[1].append(jnp.where(top, pltpu.roll(a, 4, 0), b))
        return [jnp.concatenate(half, axis=0) for half in halves]

    def update(halves, alpha, beta):
        total = jnp.zeros((q_all, BLK), F32)
        for h in range(2):
            stack = []
            for s in range(4):
                stack += pieces(jnp.where(band == s, halves[h], 0.0))
            found = nn(jnp.concatenate(stack, axis=0), cst[h])
            for s in range(4):
                lifted = found[2 * s * q_all : (2 * s + 1) * q_all] + found[(2 * s + 1) * q_all : (2 * s + 2) * q_all]
                at = 4 * h + s
                lifted = lifted + beta * lift[at]
                lift[at] = lifted
                image = nn((d_ref[at] + lifted).astype(BF16), kmat[at])
                residual = r_ref[at] - alpha * image
                r_ref[at] = residual
                precond = nn(residual.astype(BF16), dmat[at])
                v_ref[at] = precond
                total = total + residual * precond
        return total

    d_ref[...] = jnp.zeros(d_ref.shape, F32)
    track[...] = jnp.zeros(track.shape, F32)
    lift[...] = jnp.zeros(lift.shape, F32)
    y_old[...] = jnp.zeros(y_old.shape, F32)
    for fetch in fetches[:3]:
        fetch.wait()
    build_tables()
    local_partials()
    for fetch in fetches[3:5]:
        fetch.wait()
    total = jnp.zeros((q_all, BLK), F32)
    for s in range(subs):
        total = total + r_ref[s] * nn(r_ref[s].astype(BF16), dmat[s])
    first_row = as_row(total)
    part = max(2, nb // 2)
    for fetch in fetches[5 : 5 + part // 2]:
        fetch.wait()
    invert_blocks(0, part)
    pl.semaphore_wait(barrier, n_mem + n_grp - 2)
    for step in reversed(order[1:]):
        to_member(idx, idx_all.at[me], sem_i, step).start()
    send_partials()
    idx_all[pl.ds(me, 1)] = idx[...][None]

    def start_sums(norm_row):
        total = jnp.zeros((q_all, BLK), F32)
        mixed = jnp.zeros((q_all, BLK), F32)
        for s in range(subs):
            total = total + v_ref[s] * solved[s]
            mixed = mixed + v_ref[s] * track[s]
        packed = as_row(jnp.zeros((q_all, BLK), F32), total)
        reduce_start(norm_row + packed, as_row(mixed))

    start_sums(first_row)
    for fetch in fetches[5 + part // 2 :]:
        fetch.wait()
    if nb > part:
        invert_blocks(part, nb - part)
    build_masks()

    def iteration(t, before):
        norm_before, curvature_before = before
        for number in range(n_chunks):
            gather_chunk(number)
        for u in range(nb // 2):
            far_load(u).start()
        near_load().start()
        reduce_middle()
        acc = lower()
        squares = jnp.zeros((8, BLK), F32)
        crosses = jnp.zeros((8, BLK), F32)
        for i in range(nb):
            y_new[i] = acc[i]
            squares = squares + acc[i] * acc[i]
            crosses = crosses + acc[i] * y_old[i]
        found = reduce_end()
        energy_start(jnp.sum(squares, axis=1, keepdims=True), jnp.sum(crosses, axis=1, keepdims=True))
        upper(acc)
        pick_early()
        extra = energy_end()
        for u in range(nb // 2):
            far_spread(u).wait()
        for number in reversed(range(n_chunks)):
            pick_chunk(number, extra)
        norm_now = found[0:1]
        beta = jnp.where(t == 0, 0.0, norm_now / norm_before)
        beta_column = as_column(beta)
        my_beta = as_my_column(beta)
        for s in range(subs):
            d_ref[s] = v_ref[s] + beta_column * d_ref[s]
            track[s] = solved[s] + beta_column * track[s]
        for i in range(nb):
            y_old[i] = y_new[i] + my_beta * y_old[i]
        plain = as_column(norm_now, q_all)
        mixed = 2.0 * as_column(found[1:2]) + beta_column * curvature_before
        plain = plain + beta_column * mixed
        norm_column = as_column(norm_now)
        halves = picked()
        curvature = plain + (
            halves[0][:, corners : corners + 1] + 2.0 * beta_column * halves[0][:, corners + 1 : corners + 2]
        )
        alpha = norm_column / curvature
        norm_row = as_row(update(halves, alpha, beta_column))
        rows_ref[pl.ds(t, 1), :] = back_to_row(alpha)

        @pl.when(t < ITERS - 1)
        def _():
            local_partials()
            send_partials()
            start_sums(norm_row)

        @pl.when(t == ITERS - 1)
        def _():
            reduce_start(norm_row)

        return norm_now, curvature

    start = (jnp.ones((1, 128), F32), jnp.zeros((q_all, 1), F32))
    norm_before, _ = lax.fori_loop(0, ITERS, iteration, start)
    leaving = [
        pltpu.make_async_copy(src, dst, sem_o.at[number])
        for number, (src, dst) in enumerate(((r_ref, r_out), (v_ref, v_out), (d_ref, d_out)))
    ]
    for copy in leaving:
        copy.start()
    reduce_middle()
    rows_ref[ITERS : ITERS + 1, :] = reduce_end()[0:1] / norm_before
    for copy in leaving:
        copy.wait()


def finish(r_in, v_in, d_in, rows_in, r_out, d_out, steps_out, r_ref, v_ref, d_ref, rows, sem):
    subs, q_all, _ = r_ref.shape
    copies = [
        pltpu.make_async_copy(src, dst, sem.at[number])
        for number, (src, dst) in enumerate(
            ((v_in, v_ref), (d_in, d_ref), (rows_in, rows), (r_in, r_ref), (r_ref, r_out), (d_ref, d_out))
        )
    ]
    for copy in copies[:4]:
        copy.start()
    for copy in copies[:3]:
        copy.wait()
    diagonal = iota((q_all, 128), 0) == iota((q_all, 128), 1)
    beta = jnp.broadcast_to(rows[ITERS : ITERS + 1, :], (q_all, 128))
    beta = jnp.sum(jnp.where(diagonal, beta, 0.0), axis=1, keepdims=True)
    for s in range(subs):
        d_ref[s] = v_ref[s] + beta * d_ref[s]
    copies[5].start()
    copies[3].wait()
    copies[4].start()
    steps_out[...] = rows[0:ITERS, 0:q_all]
    copies[5].wait()
    copies[4].wait()


def local(n_grp, n_mem, residual, direction, local_inverse, dirichlet, coupling, corner_map, coarse_factor):
    subs, q_all, nr = residual.shape
    order = coarse_factor.shape[1]
    nb = order // BLK
    n_rows = 12 * nb
    most = max(n_mem, n_grp)
    dma = pltpu.SemaphoreType.DMA
    vmem = pl.BlockSpec(memory_space=pltpu.VMEM)
    anywhere = pl.BlockSpec(memory_space=pltpu.HBM)
    field = pltpu.VMEM(residual.shape, F32)
    tiles = pltpu.VMEM((n_mem, 8, 128), F32)
    whole = jax.ShapeDtypeStruct(residual.shape, F32)
    fields = pl.pallas_call(
        functools.partial(kernel, n_grp, n_mem),
        out_shape=(whole, whole, whole, jax.ShapeDtypeStruct((8, 128), F32)),
        in_specs=[anywhere] * 5 + [vmem, anywhere],
        out_specs=(anywhere,) * 3 + (vmem,),
        scratch_shapes=[
            field,
            field,
            field,
            pltpu.VMEM(local_inverse.shape, BF16),
            pltpu.VMEM(dirichlet.shape, BF16),
            pltpu.VMEM(coupling.shape, BF16),
            pltpu.VMEM((2, 128, nr), BF16),
            field,
            field,
            field,
            pltpu.VMEM((order, order), BF16),
            pltpu.VMEM((nb // 2, 3, BLK, BLK), BF16),
            pltpu.VMEM((nb // 2, 3, BLK, BLK), BF16),
            pltpu.VMEM((BLK, n_mem * BLK), BF16),
            pltpu.VMEM((n_rows, n_mem * BLK), F32),
            pltpu.VMEM((2 * n_rows, n_mem * BLK), BF16),
            pltpu.VMEM((8, 128), jnp.int32),
            tiles,
            tiles,
            tiles,
            tiles,
            pltpu.VMEM((n_mem, 8, 128), jnp.int32),
            pltpu.VMEM((n_rows, BLK), F32),
            pltpu.VMEM((2, 4 * nb, BLK), F32),
            pltpu.VMEM((n_rows, BLK), F32),
            pltpu.VMEM((8, n_mem * BLK), F32),
            pltpu.VMEM((nb, 8, BLK), F32),
            pltpu.VMEM((nb, 8, BLK), F32),
            pltpu.VMEM((2, most, 2, 128), F32),
            pltpu.VMEM((n_grp, 1, 128), F32),
            dma((4 + nb,)),
            dma((3,)),
            dma((2, n_mem)),
            dma((2, n_mem)),
            dma((2, n_mem)),
            dma((2, nb // 2 + 1)),
            dma((2, nb // 2 + 1)),
            dma((2, 2, most)),
            dma((2, n_grp)),
        ],
        compiler_params=pltpu.CompilerParams(
            collective_id=0, has_side_effects=True, vmem_limit_bytes=VMEM_LIMIT
        ),
    )(residual, direction, local_inverse, dirichlet, coupling, corner_map, coarse_factor)
    return pl.pallas_call(
        finish,
        out_shape=(whole, whole, jax.ShapeDtypeStruct((ITERS, q_all), F32)),
        in_specs=[anywhere] * 4,
        out_specs=(anywhere, anywhere, vmem),
        scratch_shapes=[field, field, field, pltpu.VMEM((8, 128), F32), dma((6,))],
        compiler_params=pltpu.CompilerParams(vmem_limit_bytes=VMEM_LIMIT),
    )(*fields)


def solution(mesh):
    both = ("grp", "mem")
    return jax.shard_map(
        functools.partial(local, mesh.shape["grp"], mesh.shape["mem"]),
        mesh=mesh,
        in_specs=(P(both), P(both), P(both), P(both), P(both), P(both), P("grp")),
        out_specs=(P(both), P(both), P()),
        check_vma=False,
    )
```

```python
import functools

import jax
import jax.numpy as jnp
from jax import lax
from jax.experimental import pallas as pl
from jax.experimental.pallas import tpu as pltpu
from jax.sharding import PartitionSpec as P

ITERS = 3
MESH = pl.DeviceIdType.MESH
F32, BF16 = jnp.float32, jnp.bfloat16
BLK = 256
WIDE = 4
VMEM_LIMIT = 50 * 1024 * 1024


def nn(a, b):
    return lax.dot_general(a, b, (((1,), (0,)), ((), ())), preferred_element_type=F32)


def nt(a, b):
    return lax.dot_general(a, b, (((1,), (1,)), ((), ())), preferred_element_type=F32)


def pieces(x):
    high = x.astype(BF16)
    return high, (x - high.astype(F32)).astype(BF16)


def iota(shape, dim):
    return lax.broadcasted_iota(jnp.int32, shape, dim)


def kernel(
    n_grp, n_mem,
    r_in, d_in, kmat_in, dmat_in, coupling_in, corner_in, factor,
    r_out, v_out, d_out, rows_ref,
    r_ref, v_ref, d_ref, corner_map, kmat, dmat, coupling, cst, solved, track, lift, l_ref, xh, xl, oht, mask, a_ref,
    idx, snd, rcv, snd2, rcv2, idx_all, load, nbr, ext, sums, y_new, y_old, ar, energy,
    sem_l, sem_o, sem_i, sem_f, sem_b, sem_n, sem_x, sem_a, sem_e,
):
    subs, q_all, _ = r_in.shape
    corners = coupling_in.shape[1]
    nb = l_ref.shape[0] // BLK
    rows4 = 4 * nb
    wide = min(WIDE, nb)
    n_rows = 3 * rows4
    me, grp = lax.axis_index("mem"), lax.axis_index("grp")
    top = iota((8, 128), 0) < 4
    top2 = iota((8, BLK), 0) < 4
    band = iota((q_all, 128), 1) // 32
    order = [0]
    for near in range(1, n_mem // 2):
        order += [near, n_mem - near]
    order.append(n_mem // 2)
    chunk = min(4, n_mem)
    n_chunks = n_mem // chunk
    even = lax.rem(grp, 2) == 0
    near_step = jnp.where(even, 1, n_grp - 1)
    far_step = jnp.where(even, n_grp - 1, 1)

    side = lax.rem(grp // 2, 2)
    across = me + 1 - 2 * lax.rem(me, 2)

    def member_at(step):
        return lax.rem(me + step, n_mem)

    def flip(member):
        return member + side * (1 - 2 * lax.rem(member, 2))

    mine = flip(me)

    def same_rows(step):
        other = lax.rem(grp + step, n_grp)
        turn = lax.rem(other // 2, 2) - side
        return {"grp": other, "mem": me + turn * turn * (1 - 2 * lax.rem(me, 2))}

    def span(u, count):
        return pl.ds(2 * BLK * u, 2 * BLK * count)

    fetches = [
        pltpu.make_async_copy(src, dst, sem_l.at[number])
        for number, (src, dst) in enumerate(
            [(d_in, v_ref), (kmat_in, kmat), (coupling_in, coupling), (corner_in, corner_map), (r_in, r_ref), (dmat_in, dmat)]
            + [(factor.at[0, span(u, 1), span(u, 1)], l_ref.at[span(u, 1), span(u, 1)]) for u in range(nb // 2)]
            + [
                (factor.at[0, span(u + 1, nb // 2 - u - 1), span(u, 1)], l_ref.at[span(u + 1, nb // 2 - u - 1), span(u, 1)])
                for u in range(nb // 2 - 1)
            ]
        )
    ]
    for fetch in fetches[:4]:
        fetch.start()

    barrier = pltpu.get_barrier_semaphore()
    for step in range(1, n_mem):
        pl.semaphore_signal(barrier, inc=1, device_id={"mem": member_at(step)}, device_id_type=MESH)
    for step in range(1, n_grp):
        pl.semaphore_signal(barrier, inc=1, device_id=same_rows(step), device_id_type=MESH)

    def to_member(src, dst, sem, step):
        return pltpu.make_async_remote_copy(
            src_ref=src, dst_ref=dst, send_sem=sem.at[0, step], recv_sem=sem.at[1, step],
            device_id={"mem": lax.rem(me + step, n_mem)}, device_id_type=MESH,
        )

    def to_group(src, dst, sem, step):
        return pltpu.make_async_remote_copy(
            src_ref=src, dst_ref=dst, send_sem=sem.at[0, step], recv_sem=sem.at[1, step],
            device_id=same_rows(step), device_id_type=MESH,
        )

    def to_neighbour(src, dst, sem, number, step, member):
        return pltpu.make_async_remote_copy(
            src_ref=src, dst_ref=dst, send_sem=sem.at[0, number], recv_sem=sem.at[1, number],
            device_id={"grp": lax.rem(grp + step, n_grp), "mem": member}, device_id_type=MESH,
        )

    def near_load():
        return to_neighbour(load.at[0:rows4], nbr.at[0], sem_n, nb // 2, near_step, me)

    def far_load(u):
        piece = pl.ds(8 * u, 8)
        return to_neighbour(load.at[pl.ds(2 * rows4 + 8 * u, 8)], nbr.at[1, piece], sem_n, u, far_step, across)

    def near_spread():
        return to_neighbour(ext.at[rows4 : 2 * rows4], ext.at[0:rows4], sem_x, nb // 2, near_step, me)

    def far_spread(u):
        return to_neighbour(
            ext.at[pl.ds(rows4 + 8 * u, 8)], ext.at[pl.ds(2 * rows4 + 8 * u, 8)], sem_x, u, far_step, across
        )

    def reduce_start(parity, *rows):
        first = ar.at[parity, 0]
        for number, row in enumerate(rows):
            first[pl.ds(me, 1), number : number + 1, :] = row[None]
        for step in reversed(order[1:]):
            to_member(first.at[me], first.at[me], sem_a.at[parity, 0], step).start()

    def reduce_middle(parity):
        first, second = ar.at[parity, 0], ar.at[parity, 1]
        for step in range(1, n_mem):
            to_member(first.at[me], first.at[member_at(n_mem - step)], sem_a.at[parity, 0], step).wait()
        second[pl.ds(grp, 1)] = jnp.sum(first[0:n_mem], axis=0)[None]
        for step in range(1, n_grp):
            to_group(second.at[grp], second.at[grp], sem_a.at[parity, 1], step).start()

    def reduce_end(parity):
        second = ar.at[parity, 1]
        for step in range(1, n_grp):
            source = second.at[lax.rem(grp + n_grp - step, n_grp)]
            to_group(second.at[grp], source, sem_a.at[parity, 1], step).wait()
        return jnp.sum(second[0:n_grp], axis=0)

    def energy_start(parity, squares, crosses):
        place = iota((8, 128), 0) == iota((8, 128), 1)
        column = jnp.where(top, jnp.broadcast_to(squares, (8, 128)), jnp.broadcast_to(crosses, (8, 128)))
        slots = energy.at[parity]
        slots[pl.ds(grp, 1)] = jnp.sum(jnp.where(place, column, 0.0), axis=0, keepdims=True)[None]
        for step in range(1, n_grp):
            to_group(slots.at[grp], slots.at[grp], sem_e.at[parity], step).start()

    def energy_end(parity):
        slots = energy.at[parity]
        for step in range(1, n_grp):
            source = slots.at[lax.rem(grp + n_grp - step, n_grp)]
            to_group(slots.at[grp], source, sem_e.at[parity], step).wait()
        row = jnp.sum(slots[...], axis=0)
        place = iota((8, 128), 0) == iota((8, 128), 1)
        column = jnp.sum(jnp.where(place, jnp.broadcast_to(row, (8, 128)), 0.0), axis=1, keepdims=True)
        column = jnp.broadcast_to(column, (8, 128))
        return jnp.where(iota((8, 128), 1) == corners, column, pltpu.roll(column, 4, 0))

    def as_row(*totals):
        spare = 128 - q_all * len(totals)
        fill = [jnp.zeros((spare, BLK), F32)] if spare else []
        wide = jnp.concatenate([*totals, *fill], axis=0)
        first = wide.astype(BF16)
        rest = wide - first.astype(F32)
        second = rest.astype(BF16)
        third = (rest - second.astype(F32)).astype(BF16)
        ones = jnp.ones((8, BLK), BF16)
        out = nt(ones, first) + (nt(ones, second) + nt(ones, third))
        return out[0:1]

    def as_column(row, offset=0):
        diagonal = iota((q_all, 128), 0) + offset == iota((q_all, 128), 1)
        return jnp.sum(jnp.where(diagonal, jnp.broadcast_to(row, (q_all, 128)), 0.0), axis=1, keepdims=True)

    def back_to_row(column):
        diagonal = iota((q_all, 128), 0) == iota((q_all, 128), 1)
        return jnp.sum(jnp.where(diagonal, jnp.broadcast_to(column, (q_all, 128)), 0.0), axis=0, keepdims=True)

    mine4 = iota((8, 128), 1) == 4 * mine + lax.rem(iota((8, 128), 0), 4)

    def as_my_column(row):
        return jnp.sum(jnp.where(mine4, jnp.broadcast_to(row, (8, 128)), 0.0), axis=1, keepdims=True)

    def build_tables():
        cst[...] = jnp.zeros(cst.shape, BF16)
        for s in range(subs):
            cst[s // 4, 32 * (s % 4) : 32 * (s % 4) + corners, :] = coupling[s]
        idx[...] = jnp.full((8, 128), -1, jnp.int32)
        idx[:, 0:corners] = corner_map[...]
        wide = idx[...]
        lane, sub = iota((8, 128), 1) // 32, iota((8, 128), 0)
        tile = jnp.full((8, 128), -1, jnp.int32)
        for s in range(subs):
            turned = pltpu.roll(wide, 32 * (s % 4), 1)[s : s + 1] if s % 4 else wide[s : s + 1]
            tile = jnp.where((lane == s % 4) & (sub // 4 == s // 4), jnp.broadcast_to(turned, (8, 128)), tile)
        idx[...] = tile

    def local_partials():
        halves = []
        for h in range(2):
            stack = []
            for s in range(4 * h, 4 * h + 4):
                out = nn(v_ref[s].astype(BF16), kmat[s])
                solved[s] = out
                stack += pieces(out)
            found = nt(jnp.concatenate(stack, axis=0), cst[h])
            total = jnp.zeros((q_all, 128), F32)
            for s in range(4):
                part = found[2 * s * q_all : (2 * s + 1) * q_all] + found[(2 * s + 1) * q_all : (2 * s + 2) * q_all]
                total = jnp.where(band == s, part, total)
            halves.append(total)
        for v in range(q_all // 8):
            a, b = halves[0][8 * v : 8 * v + 8], halves[1][8 * v : 8 * v + 8]
            snd[2 * v] = jnp.where(top, a, pltpu.roll(b, 4, 0))
            snd[2 * v + 1] = jnp.where(top, pltpu.roll(a, 4, 0), b)

    def send_partials():
        for step in reversed(order[1:]):
            to_member(snd.at[flip(member_at(step))], rcv.at[me], sem_f, step).start()
        rcv[pl.ds(me, 1)] = snd[pl.ds(mine, 1)]

    def block(i, j):
        return l_ref[i * BLK : (i + 1) * BLK, j * BLK : (j + 1) * BLK]

    half = BLK // 2

    def between(high, low, off, high_after, low_after):
        left = nn(jnp.concatenate([high, low], axis=1), jnp.concatenate([off, off], axis=0))
        left = jnp.concatenate(pieces(left), axis=1)
        after = jnp.concatenate(
            [
                jnp.concatenate([high_after, low_after], axis=1),
                jnp.concatenate([high_after, jnp.zeros_like(low_after)], axis=1),
            ],
            axis=0,
        )
        out = nn(left, after)
        return out[:, :half] + out[:, half:]

    def invert_blocks(first, count):
        row, col = iota((half, half), 0), iota((half, half), 1)
        numbers = range(2 * first, 2 * (first + count))

        def tile(i, j):
            return l_ref[i * half : (i + 1) * half, j * half : (j + 1) * half]

        inverses = []
        for i in numbers:
            tri = tile(i, i).astype(F32)
            diag = jnp.where(row == col, tri, 0.0)
            down = 1.0 / jnp.sum(diag, axis=1, keepdims=True)
            along = 1.0 / jnp.sum(diag, axis=0, keepdims=True)
            below = (row // 2 == col // 2) & (row > col)
            inverses.append(jnp.where(row == col, down, 0.0) - jnp.where(below, tri * down * along, 0.0))
        size = 2
        while size < half:
            below = (row // (2 * size) == col // (2 * size)) & (row // size > col // size)
            split = [pieces(inv) for inv in inverses]
            offs = [jnp.where(below, tile(i, i).astype(F32), 0.0).astype(BF16) for i in numbers]
            inverses = [
                inv - between(*pair, off, *pair) for inv, pair, off in zip(inverses, split, offs)
            ]
            size *= 2
        split = [pieces(inv) for inv in inverses]
        nothing = jnp.zeros((half, half), BF16)
        for number in range(count):
            i = first + number
            before, after = split[2 * number], split[2 * number + 1]
            corner = pieces(-between(*after, tile(2 * i + 1, 2 * i), *before))
            for ref, a, b, c in zip((xh, xl), before, after, corner):
                ref[i // wide, i % wide, i % wide, :half, :half] = a
                ref[i // wide, i % wide, i % wide, :half, half:] = nothing
                ref[i // wide, i % wide, i % wide, half:, :half] = c
                ref[i // wide, i % wide, i % wide, half:, half:] = b

    def merge_blocks(width):
        if 2 * width <= wide:
            for h in range(nb // wide):
                for low in range(0, wide, 2 * width):
                    mid, end = low + width, low + 2 * width
                    inner = {}
                    for i in range(mid, end):
                        for j in range(low, mid):
                            total = None
                            for k in range(j, mid):
                                off = block(h * wide + i, h * wide + k)
                                part = nn(off, xh[h, k, j]) + nn(off, xl[h, k, j])
                                total = part if total is None else total + part
                            inner[i, j] = pieces(total)
                    for i in range(mid, end):
                        for j in range(low, mid):
                            total = None
                            for k in range(mid, i + 1):
                                high, rest = inner[k, j]
                                part = nn(xh[h, i, k], high) + (nn(xh[h, i, k], rest) + nn(xl[h, i, k], high))
                                total = part if total is None else total + part
                            xh[h, i, j], xl[h, i, j] = pieces(-total)

    def build_masks():
        for step in range(1, n_mem):
            to_member(idx, idx_all.at[member_at(n_mem - step)], sem_i, step).wait()
        for position, step in enumerate(order):
            tile = idx_all[pl.ds(member_at(n_mem - step), 1)][0]
            for h in range(2):
                line = tile[4 * h : 4 * h + 1]
                at = position * BLK + h * 128
                lo = jnp.broadcast_to(line & (BLK - 1), (BLK, 128))
                oht[:, at : at + 128] = jnp.where(lo == iota((BLK, 128), 0), 1.0, 0.0).astype(BF16)
                below, above = jnp.where(even, 2 * nb, 0), jnp.where(even, 0, 2 * nb)
                hi = line >> 8
                moved = jnp.where(hi < nb, hi + below, jnp.where(hi < 2 * nb, hi, hi - 2 * nb + above))
                hi = jnp.broadcast_to(jnp.where(hi < 0, -1, moved), (n_rows, 128))
                mask[:, at : at + 128] = jnp.where(hi == iota((n_rows, 128), 0) // 4, 1.0, 0.0)

    def gather_chunk(number):
        positions = range(number * chunk, (number + 1) * chunk)
        for position in positions:
            step = order[position]
            if step:
                to_member(snd.at[flip(member_at(step))], rcv.at[member_at(n_mem - step)], sem_f, step).wait()
        for position in positions:
            tile = rcv[pl.ds(member_at(n_mem - order[position]), 1)][0]
            high = tile.astype(BF16).astype(F32)
            for number_of, part in enumerate((high, tile - high)):
                turned = pltpu.roll(part, 4, 0)
                for h in range(2):
                    twice = jnp.where(top, part, turned) if h == 0 else jnp.where(top, turned, part)
                    at = position * BLK + h * 128
                    full = jnp.concatenate([twice] * (n_rows // 8), axis=0) * mask[:, at : at + 128]
                    a_ref[number_of * n_rows : (number_of + 1) * n_rows, at : at + 128] = full.astype(BF16)
        at = slice(number * chunk * BLK, (number + 1) * chunk * BLK)
        total = nt(a_ref[:, at], oht[:, at])
        total = total[:n_rows] + total[n_rows:]
        load[...] = total if number == 0 else load[...] + total

    def twin(x):
        high, low = pieces(x)
        return jnp.where(top2, high.astype(F32), low.astype(F32)).astype(BF16)

    def folded(x):
        return x + pltpu.roll(x, 4, 0)

    def inverse(i, j):
        place = (i // wide, i % wide, j % wide)
        return xh[place], xl[place]

    def both(product, left, i, j):
        high, low = inverse(i, j)
        return product(left, high) + product(left, low)

    def lower(wide):
        acc, taken = [], [None] * nb
        near_load().wait()
        for h in range(nb // wide):
            base = h * wide
            right = []
            for u in range(base // 2, (base + wide) // 2):
                far_load(u).wait()
            for u in range(base // 2, (base + wide) // 2):
                piece = slice(8 * u, 8 * u + 8)
                x = load[rows4 + 8 * u : rows4 + 8 * u + 8] + nbr[0, piece] + nbr[1, piece]
                y = pltpu.roll(x, 4, 0)
                right += [jnp.where(top2, x, y), jnp.where(top2, y, x)]
            if h:
                right = [b - folded(taken[base + i]) for i, b in enumerate(right)]
            right = [twin(b) for b in right]
            found = []
            for i in range(wide):
                total = None
                for j in range(i + 1):
                    part = both(nt, right[j], base + i, base + j)
                    total = part if total is None else total + part
                found.append(folded(total))
            acc += found
            found = [twin(y) for y in found]
            for t in range(base + wide, nb):
                for j in range(wide):
                    part = nt(found[j], block(t, base + j))
                    taken[t] = part if taken[t] is None else taken[t] + part
        for i in range(nb):
            y_new[i] = acc[i]

    def upper(wide):
        acc = [y_new[i] for i in range(nb)]
        for h in reversed(range(nb // wide)):
            base = h * wide
            right = [twin(acc[base + i]) for i in range(wide)]
            found = [None] * wide
            for j in reversed(range(wide)):
                total = None
                for i in range(j, wide):
                    part = both(nn, right[i], base + i, base + j)
                    total = part if total is None else total + part
                found[j] = folded(total)
            for u in range(base // 2, (base + wide) // 2):
                i = 2 * u - base
                ext[rows4 + 8 * u : rows4 + 8 * u + 8] = jnp.where(top2, found[i], found[i + 1])
                far_spread(u).start()
            found = [twin(x) for x in found]
            for t in range(base):
                total = None
                for j in range(wide):
                    part = nn(found[j], block(base + j, t))
                    total = part if total is None else total + part
                acc[t] = acc[t] - folded(total)
        near_spread().start()

    def far_wait():
        for u in range(nb // 2):
            far_spread(u).wait()

    def pick_rows(role, number):
        rows = slice(role * rows4, (role + 1) * rows4)
        at = slice(number * chunk * BLK, (number + 1) * chunk * BLK)
        high, low = pieces(ext[rows])
        found = nn(jnp.concatenate([high, low], axis=0), oht[:, at])
        found = (found[:rows4] + found[rows4:]) * mask[rows, at]
        total = found[0:8]
        for v in range(1, rows4 // 8):
            total = total + found[8 * v : 8 * v + 8]
        return total

    def pick_early():
        for number in range(n_chunks):
            sums[:, number * chunk * BLK : (number + 1) * chunk * BLK] = pick_rows(1, number)
        near_spread().wait()
        for number in range(n_chunks):
            at = slice(number * chunk * BLK, (number + 1) * chunk * BLK)
            sums[:, at] = sums[:, at] + pick_rows(0, number)

    def pick_chunk(number, extra):
        at = slice(number * chunk * BLK, (number + 1) * chunk * BLK)
        total = sums[:, at] + pick_rows(2, number)
        total = total + pltpu.roll(total, 4, 0)
        steps = []
        padding = top & (iota((8, 128), 1) // 2 == corners // 2)
        for position in range(chunk):
            step = (n_mem - order[number * chunk + position]) % n_mem
            begin = position * BLK
            tile = jnp.where(top, total[:, begin : begin + 128], total[:, begin + 128 : begin + 256])
            tile = jnp.where(padding, extra, tile)
            if step:
                snd2[pl.ds(member_at(step), 1)] = tile[None]
                steps.append(step)
            else:
                rcv2[pl.ds(mine, 1)] = tile[None]
        for step in reversed(steps):
            to_member(snd2.at[member_at(step)], rcv2.at[mine], sem_b, step).start()

    def picked():
        for step in order[1:]:
            to_member(snd2.at[member_at(step)], rcv2.at[flip(member_at(n_mem - step))], sem_b, step).wait()
        halves = ([], [])
        for v in range(q_all // 8):
            a, b = rcv2[2 * v], rcv2[2 * v + 1]
            halves[0].append(jnp.where(top, a, pltpu.roll(b, 4, 0)))
            halves[1].append(jnp.where(top, pltpu.roll(a, 4, 0), b))
        return [jnp.concatenate(half, axis=0) for half in halves]

    def update(halves, alpha, beta, t):
        total = jnp.zeros((q_all, BLK), F32)
        for h in range(2):
            stack = []
            for s in range(4):
                stack += pieces(jnp.where(band == s, halves[h], 0.0))
            found = nn(jnp.concatenate(stack, axis=0), cst[h])
            for s in range(4):
                lifted = found[2 * s * q_all : (2 * s + 1) * q_all] + found[(2 * s + 1) * q_all : (2 * s + 2) * q_all]
                at = 4 * h + s
                lifted = lifted + jnp.where(t == 0, 0.0, beta * lift[at])
                lift[at] = lifted
                image = nn((d_ref[at] + lifted).astype(BF16), kmat[at])
                residual = r_ref[at] - alpha * image
                r_ref[at] = residual
                precond = nn(residual.astype(BF16), dmat[at])
                v_ref[at] = precond
                total = total + residual * precond
        return total

    y_old[...] = jnp.zeros(y_old.shape, F32)
    for fetch in fetches[:4]:
        fetch.wait()
    for fetch in fetches[4:]:
        fetch.start()
    build_tables()
    local_partials()
    part = max(2, nb // 2)
    pl.semaphore_wait(barrier, n_mem + n_grp - 2)
    for step in reversed(order[1:]):
        to_member(idx, idx_all.at[me], sem_i, step).start()
    send_partials()
    idx_all[pl.ds(me, 1)] = idx[...][None]

    def start_sums(parity, norm, first=False):
        total = jnp.zeros((q_all, BLK), F32)
        mixed = jnp.zeros((q_all, BLK), F32)
        for s in range(subs):
            total = total + v_ref[s] * solved[s]
            if not first:
                mixed = mixed + v_ref[s] * track[s]
        reduce_start(parity, as_row(norm, total), as_row(mixed))

    for fetch in fetches[4:6]:
        fetch.wait()
    first_norm = jnp.zeros((q_all, BLK), F32)
    for s in range(subs):
        first_norm = first_norm + r_ref[s] * nn(r_ref[s].astype(BF16), dmat[s])
    start_sums(0, first_norm, True)
    for fetch in fetches[6:]:
        fetch.wait()
    for first in range(0, nb, part):
        invert_blocks(first, part)
    build_masks()

    def iteration(t, before):
        norm_before, curvature_before = before
        for number in range(n_chunks):
            gather_chunk(number)
        for u in range(nb // 2):
            far_load(u).start()
        near_load().start()
        reduce_middle(lax.rem(t, 2))

        @pl.when(t == 0)
        def _():
            merge_blocks(1)
            lower(2)

        @pl.when(t > 0)
        def _():
            lower(wide)

        squares = jnp.zeros((8, BLK), F32)
        crosses = jnp.zeros((8, BLK), F32)
        for i in range(nb):
            squares = squares + y_new[i] * y_new[i]
            crosses = crosses + y_new[i] * y_old[i]
        energy_start(lax.rem(t, 2), jnp.sum(squares, axis=1, keepdims=True), jnp.sum(crosses, axis=1, keepdims=True))

        @pl.when(t == 0)
        def _():
            upper(2)

        @pl.when(t > 0)
        def _():
            upper(wide)

        pick_early()
        far_wait()
        extra = energy_end(lax.rem(t, 2))
        for number in reversed(range(n_chunks)):
            pick_chunk(number, extra)

        @pl.when(t == 0)
        def _():
            merge_blocks(2)

        found = reduce_end(lax.rem(t, 2))
        norm_now = found[0:1]
        beta = jnp.where(t == 0, 0.0, norm_now / norm_before)
        beta_column = as_column(beta)
        my_beta = as_my_column(beta)
        for s in range(subs):
            d_ref[s] = v_ref[s] + jnp.where(t == 0, 0.0, beta_column * d_ref[s])
            track[s] = solved[s] + jnp.where(t == 0, 0.0, beta_column * track[s])
        for i in range(nb):
            y_old[i] = y_new[i] + my_beta * y_old[i]
        plain = as_column(norm_now, q_all)
        mixed = 2.0 * as_column(found[1:2]) + beta_column * curvature_before
        plain = plain + beta_column * mixed
        norm_column = as_column(norm_now)
        halves = picked()
        curvature = plain + (
            halves[0][:, corners : corners + 1] + 2.0 * beta_column * halves[0][:, corners + 1 : corners + 2]
        )
        alpha = norm_column / curvature
        norm = update(halves, alpha, beta_column, t)

        @pl.when(t < ITERS - 1)
        def _():
            local_partials()
            send_partials()
            start_sums(lax.rem(t + 1, 2), norm)

        @pl.when(t == ITERS - 1)
        def _():
            reduce_start(ITERS % 2, as_row(norm))

        rows_ref[pl.ds(t, 1), :] = back_to_row(alpha)
        return norm_now, curvature

    start = (jnp.ones((1, 128), F32), jnp.zeros((q_all, 1), F32))
    norm_before, _ = lax.fori_loop(0, ITERS, iteration, start)
    leaving = [
        pltpu.make_async_copy(src, dst, sem_o.at[number])
        for number, (src, dst) in enumerate(((r_ref, r_out), (v_ref, v_out), (d_ref, d_out)))
    ]
    for copy in leaving:
        copy.start()
    reduce_middle(ITERS % 2)
    rows_ref[ITERS : ITERS + 1, :] = reduce_end(ITERS % 2)[0:1] / norm_before
    for copy in leaving:
        copy.wait()


def finish(r_in, v_in, d_in, rows, r_out, d_out, steps_out, d_ref, sem):
    subs, q_all, _ = d_ref.shape
    rest = pltpu.make_async_copy(r_in, r_out, sem.at[0])
    rest.start()
    diagonal = iota((q_all, 128), 0) == iota((q_all, 128), 1)
    beta = jnp.broadcast_to(rows[ITERS : ITERS + 1, :], (q_all, 128))
    beta = jnp.sum(jnp.where(diagonal, beta, 0.0), axis=1, keepdims=True)
    for s in range(subs):
        d_ref[s] = v_in[s] + beta * d_in[s]
    moved = pltpu.make_async_copy(d_ref, d_out, sem.at[1])
    moved.start()
    steps_out[...] = rows[0:ITERS, 0:q_all]
    rest.wait()
    moved.wait()


def local(n_grp, n_mem, residual, direction, local_inverse, dirichlet, coupling, corner_map, coarse_factor):
    subs, q_all, nr = residual.shape
    order = coarse_factor.shape[1]
    nb = order // BLK
    n_rows = 12 * nb
    most = max(n_mem, n_grp)
    dma = pltpu.SemaphoreType.DMA
    vmem = pl.BlockSpec(memory_space=pltpu.VMEM)
    anywhere = pl.BlockSpec(memory_space=pltpu.HBM)
    field = pltpu.VMEM(residual.shape, F32)
    wide = min(WIDE, nb)
    inverse = pltpu.VMEM((nb // wide, wide, wide, BLK, BLK), BF16)
    tiles = pltpu.VMEM((n_mem, 8, 128), F32)
    whole = jax.ShapeDtypeStruct(residual.shape, F32)
    operands = (residual, direction, local_inverse, dirichlet, coupling, corner_map, coarse_factor)
    fields = pl.pallas_call(
        functools.partial(kernel, n_grp, n_mem),
        out_shape=(whole, whole, whole, jax.ShapeDtypeStruct((8, 128), F32)),
        in_specs=[anywhere] * 7,
        out_specs=(anywhere,) * 3 + (vmem,),
        scratch_shapes=[
            field,
            field,
            field,
            pltpu.VMEM(corner_map.shape, jnp.int32),
            pltpu.VMEM(local_inverse.shape, BF16),
            pltpu.VMEM(dirichlet.shape, BF16),
            pltpu.VMEM(coupling.shape, BF16),
            pltpu.VMEM((2, 128, nr), BF16),
            field,
            field,
            field,
            pltpu.VMEM((order, order), BF16),
            inverse,
            inverse,
            pltpu.VMEM((BLK, n_mem * BLK), BF16),
            pltpu.VMEM((n_rows, n_mem * BLK), F32),
            pltpu.VMEM((2 * n_rows, n_mem * BLK), BF16),
            pltpu.VMEM((8, 128), jnp.int32),
            tiles,
            tiles,
            tiles,
            tiles,
            pltpu.VMEM((n_mem, 8, 128), jnp.int32),
            pltpu.VMEM((n_rows, BLK), F32),
            pltpu.VMEM((2, 4 * nb, BLK), F32),
            pltpu.VMEM((n_rows, BLK), F32),
            pltpu.VMEM((8, n_mem * BLK), F32),
            pltpu.VMEM((nb, 8, BLK), F32),
            pltpu.VMEM((nb, 8, BLK), F32),
            pltpu.VMEM((2, 2, most, 2, 128), F32),
            pltpu.VMEM((2, n_grp, 1, 128), F32),
            dma((5 + nb,)),
            dma((3,)),
            dma((2, n_mem)),
            dma((2, n_mem)),
            dma((2, n_mem)),
            dma((2, nb // 2 + 1)),
            dma((2, nb // 2 + 1)),
            dma((2, 2, 2, most)),
            dma((2, 2, n_grp)),
        ],
        compiler_params=pltpu.CompilerParams(
            collective_id=0, has_side_effects=True, vmem_limit_bytes=VMEM_LIMIT
        ),
    )(*(pltpu.with_memory_space_constraint(x, pltpu.HBM) for x in operands))
    return pl.pallas_call(
        finish,
        out_shape=(whole, whole, jax.ShapeDtypeStruct((ITERS, q_all), F32)),
        in_specs=[vmem] * 4,
        out_specs=(anywhere, anywhere, vmem),
        scratch_shapes=[field, dma((2,))],
        compiler_params=pltpu.CompilerParams(vmem_limit_bytes=VMEM_LIMIT),
    )(*fields)


def solution(mesh):
    both = ("grp", "mem")
    return jax.shard_map(
        functools.partial(local, mesh.shape["grp"], mesh.shape["mem"]),
        mesh=mesh,
        in_specs=(P(both), P(both), P(both), P(both), P(both), P(both), P("grp")),
        out_specs=(P(both), P(both), P()),
        check_vma=False,
    )
```
